512 devices in a mesh: dp: 128 (over y, x_lo, z), shard: 4 (over x_hi, core).
Axes of the slice: x: 4 (x_hi: 2, x_lo: 2; x = x_hi * 2 + x_lo), y: 4, z: 16, core: 2. Of those that a mesh axis runs over, the one named last changes fastest.
Arguments:
- hidden_acts: bfloat16 [128, 128, 8192], P('dp', None, 'shard'), may hold values from -6 to 6
- out_grad: bfloat16 [128, 128, 1024], P('dp'), may hold values from -0.0546875 to 0.0546875
- token_ids: int32 [128, 128], P('dp'), may hold values from 0 to 255999, as said below
- trigger: int32 [128, 512], P('dp', 'shard'), may hold values 0 or 1
- stale: bfloat16 [128, 8192, 1024], P('dp', 'shard'), may hold values from -0.5 to 0.5
- aggregate_prev: float32 [4, 2048, 1024], P('shard', 'dp'), may hold values from -12 to 12
Outputs:
- aggregate: float32 [4, 2048, 1024], P('shard', 'dp')
- update: float32 [4, 2048, 1024], P('shard', 'dp')
- triggered: float32 [], replicated
The draws below stay inside these ranges and needn't reach their ends.
Inputs may be any that keep to these rules, and one draw needn't show every extreme that they name: `token_ids`: id 0 marks padding and stands only after all of a worker's other tokens; at least half of each worker's 128 tokens are not padding.
All inputs are finite; a program needn't handle non-finite values. No bound on the sum of `trigger` on one device may be relied on, other than what follows from the above.
Results may differ from the reference program's by a relative error of at most 0.00051.
Values may be sent and summed in bfloat16 or wider, within the bound.
A program may use at most 64 MiB of HBM per device.

```python
import math
import jax
import jax.numpy as jnp
from jax import lax

COLS = 1024
HID = 8192
VOCAB = 256000
BLOCK = 16
TOK_DEV = 128
WORKERS = 128
N_SHARD = 4


def draw_token_ids(key, part):
    length_key = jax.random.fold_in(key, 11)
    id_key = jax.random.fold_in(key, 23)
    lengths = jax.random.randint(length_key, (WORKERS, 1), TOK_DEV // 2, TOK_DEV + 1)
    values = jax.random.randint(id_key, (WORKERS, TOK_DEV), 1, VOCAB)
    position = jnp.arange(TOK_DEV)[None, :]
    return jnp.where(position < lengths, values, 0).astype(jnp.int32)


def draw_aggregate_prev(key, part):
    array_shape = (N_SHARD, HID // N_SHARD, COLS)
    row_index = jnp.arange(HID, dtype=jnp.float32).reshape(N_SHARD, HID // N_SHARD, 1)
    scales = jnp.exp(jnp.log(3.0) * row_index / HID)
    values = jnp.clip(jax.random.normal(key, array_shape, jnp.float32), -4.0, 4.0)
    return (values * scales).astype(jnp.float32)


def draw_stale(key, part):
    common_key = jax.random.fold_in(key, 31)
    jitter_key = jax.random.fold_in(key, 47)
    column_key = jax.random.fold_in(key, 59)
    shard_rows = HID // N_SHARD
    row_place = (jnp.arange(HID) % shard_rows).astype(jnp.float32) / shard_rows
    row_amp = jnp.exp(0.5 * jnp.log(3.0) * row_place)[:, None]
    column_amp = jnp.exp(jax.random.uniform(column_key, (1, COLS), jnp.float32, math.log(0.5), math.log(1.5)))
    common = 0.057 * jnp.clip(jax.random.normal(common_key, (HID, COLS), jnp.float32), -3.0, 3.0)
    jitter = 0.01 * jnp.clip(jax.random.normal(jitter_key, (WORKERS, HID, COLS), jnp.float32), -3.0, 3.0)
    shared = common * row_amp * column_amp
    return (shared[None, :, :] + jitter).astype(jnp.bfloat16)


def set_ends(values, own_key, least, largest):
    extent = values.shape
    index_at = [jax.random.randint(jax.random.fold_in(own_key, axis), (), 0, extent[axis]) for axis in range(len(extent))]
    values = values.at[tuple(index_at)].set(least)
    longest = extent.index(max(extent))
    index_at[longest] = (index_at[longest] + 1) % extent[longest]
    return values.at[tuple(index_at)].set(largest)


def levels(rng, extent, shards, low, largest):
    loudness = 1.0
    for dim, blocks in shards:
        heights = jax.random.uniform(jax.random.fold_in(jax.random.fold_in(rng, 6), dim), (blocks,), jnp.float32, low / len(shards), largest / len(shards))
        loudness = loudness * jnp.repeat(jnp.exp(heights), extent[dim] // blocks).reshape((-1,) + (1,) * (len(extent) - 1 - dim))
    return loudness


def scatter_about(stream_key, dims, width, bound, split=(), held_as=jnp.bfloat16):
    result = jax.random.normal(stream_key, dims, jnp.float32) * width
    if len(split) > 0:
        result = levels(stream_key, dims, split, -0.22, 0.18) * result
    return jnp.clip(result, min=-bound, max=bound).astype(held_as)


def setup_inputs(seed: int = 0) -> dict:
    key_of = jax.random.split(jax.random.key(seed), 7)
    return {
        "hidden_acts": scatter_about(key_of[0], (WORKERS, TOK_DEV, HID), 1.0, 6.0, ((0, 128), (2, 4))),
        "out_grad": scatter_about(key_of[1], (WORKERS, TOK_DEV, COLS), (100 * TOK_DEV) ** -0.5, 0.0546875, ((0, 128),)),
        "token_ids": draw_token_ids(jax.random.fold_in(key_of[6], 71), 0),
        "trigger": set_ends((jax.random.randint(key_of[3], (WORKERS, HID // BLOCK), 0, 2) < 1).astype(jnp.int32), jax.random.fold_in(key_of[3], 1), 0, 1),
        "stale": draw_stale(jax.random.fold_in(key_of[6], 71), 0),
        "aggregate_prev": draw_aggregate_prev(jax.random.fold_in(key_of[6], 71), 0),
    }


clip_ratio = 0.25
epsilon = 1e-06

def reference(hidden_acts, out_grad, token_ids, trigger, stale, aggregate_prev):
    real_mask = (token_ids != 0).astype(jnp.bfloat16)
    masked = out_grad * real_mask[:, :, None]

    def accumulate(running, worker_items):
        hidden, grad_out, flags, stale_rows = worker_items
        gradient = lax.dot_general(hidden, grad_out, (((0,), (0,)), ((), ())), preferred_element_type=jnp.float32)
        row_flags = jnp.repeat(flags, BLOCK).astype(jnp.float32)[:, None]
        delta = (row_flags * (gradient - stale_rows.astype(jnp.float32))).astype(jnp.bfloat16)
        delta = lax.optimization_barrier(delta)
        return (running + delta.astype(jnp.float32), None)
    start_sum = jnp.zeros((HID, COLS), jnp.float32)
    summed, unused = lax.scan(accumulate, start_sum, (hidden_acts, masked, trigger, stale))
    aggregate = aggregate_prev + summed.reshape(N_SHARD, HID // N_SHARD, COLS)
    triggered = jnp.sum(trigger.astype(jnp.float32))
    square_total = jnp.sum(aggregate * aggregate)
    limit = clip_ratio * jnp.sqrt(jnp.asarray(HID * COLS, jnp.float32))
    clip_factor = jnp.minimum(1.0, limit / jnp.sqrt(square_total + epsilon))
    return (aggregate, aggregate * clip_factor, triggered)
```

```python
import functools

import jax
import jax.numpy as jnp
from jax import lax
from jax.experimental import pallas as pl
from jax.experimental.pallas import tpu as pltpu
from jax.sharding import PartitionSpec as P

BLOCK = 16
NY, NX, NZ = 4, 2, 16
CHUNKS = 4
MESH = pl.DeviceIdType.MESH

clip_ratio = 0.25
epsilon = 1e-06


def reduce_kernel(
    rows, cols,
    hidden_ref, grad_ref, ids_ref, trigger_ref, prev_ref, stale_ref,
    aggregate_ref, sums_ref,
    hidden_t, masked, flags, delta, y_recv, x_data, x_recv, z_data, z_mid, z_recv, squares,
    stale_sem, y_send_sem, y_recv_sem, x_send_sem, x_recv_sem, z_send_sem, z_recv_sem,
):
    tokens = hidden_ref.shape[0]
    width = cols // CHUNKS
    half = rows // (NY * NX)
    own = half // NZ
    me = lax.axis_index("dp")
    y = me // (NX * NZ)
    x = (me // NZ) % NX
    z = me % NZ
    y_right, y_left, y_far = (y + 1) % NY, (y + NY - 1) % NY, (y + 2) % NY

    def at(yy, xx, zz):
        return {"dp": yy * (NX * NZ) + xx * NZ + zz}

    right, left = at(y_right, x, z), at(y_left, x, z)
    across = at(y, 1 - x, z)

    def z_off(k):
        return (z + NZ + k) % NZ

    barrier = pltpu.get_barrier_semaphore()
    peers = [right, left, across] + [at(y, x, z_off(s * k)) for k in range(1, 5) for s in (1, -1)]
    for peer in peers:
        pl.semaphore_signal(barrier, inc=1, device_id=peer, device_id_type=MESH)

    def stale_copy(c):
        return pltpu.make_async_copy(
            stale_ref.at[:, pl.ds(pl.multiple_of(c * width, 128), width)],
            delta.at[c], stale_sem.at[c],
        )

    for c in range(CHUNKS):
        stale_copy(c).start()

    keep = jnp.broadcast_to(ids_ref[...], (tokens, tokens)).T != 0
    keep = jnp.where(keep, 1.0, 0.0)
    for c in range(CHUNKS):
        for j in range(width // 128):
            part = grad_ref[:, c * width + j * 128 : c * width + (j + 1) * 128]
            masked[c, :, j * 128 : (j + 1) * 128] = (part.astype(jnp.float32) * keep).astype(jnp.bfloat16)
    blocks = rows // BLOCK
    sent = jnp.broadcast_to(trigger_ref[...].astype(jnp.float32), (blocks, blocks)).T
    for j in range(width // 128):
        flags[:, j * 128 : (j + 1) * 128] = sent

    @pl.loop(0, rows // 128)
    def _(i):
        start = pl.multiple_of(i * 128, 128)
        hidden_t[pl.ds(start, 128), :] = hidden_ref[:, pl.ds(start, 128)].T

    squares[...] = jnp.zeros_like(squares)

    def rows_of(yy, xx):
        return pl.ds(pl.multiple_of(yy * (NX * half) + xx * half, half), half)

    def y_copy(c, m):
        yy, xx, device = (
            (y_far, 0, left), (y_far, 1, right),
            (y_left, 1, left), (y_right, 0, right),
            (y_left, 0, left), (y_right, 1, right),
        )[m]
        return pltpu.make_async_remote_copy(
            delta.at[c, rows_of(yy, xx)], y_recv.at[c, m], y_send_sem.at[c, m], y_recv_sem.at[c, m],
            device_id=device, device_id_type=MESH,
        )

    def x_copy(c):
        return pltpu.make_async_remote_copy(
            x_data.at[c, 1 - x], x_recv.at[c], x_send_sem.at[c], x_recv_sem.at[c],
            device_id=across, device_id_type=MESH,
        )

    def z_copy(c, m):
        if m < 4:
            source, to = z_data.at[c, z_off(-(m + 5))], -(m + 1)
        elif m < 7:
            source, to = z_data.at[c, z_off(m + 1)], m - 3
        elif m < 9:
            source, to = z_mid.at[c, m - 7], (-4, 4)[m - 7]
        elif m < 12:
            source, to = z_data.at[c, z_off(-(m - 8))], -(m - 8)
        else:
            source, to = z_data.at[c, z_off(m - 11)], m - 11
        return pltpu.make_async_remote_copy(
            source, z_recv.at[c, m], z_send_sem.at[c, m], z_recv_sem.at[c, m],
            device_id=at(y, x, z_off(to)), device_id_type=MESH,
        )

    tile = 256

    def compute(c):
        stale_copy(c).wait()

        @pl.loop(0, rows // tile)
        def _(g):
            start = pl.multiple_of(g * tile, tile)
            gradient = jnp.dot(
                hidden_t[pl.ds(start, tile), :], masked[c], preferred_element_type=jnp.float32
            )
            diff = gradient - delta[c, pl.ds(start, tile), :].astype(jnp.float32)
            for i in range(tile // BLOCK):
                flag = flags[pl.ds(g * (tile // BLOCK) + i, 1), :]
                delta[c, pl.ds(start + i * BLOCK, BLOCK), :] = (
                    flag * diff[i * BLOCK : (i + 1) * BLOCK]
                ).astype(jnp.bfloat16)

    def send_first(c):
        for m in range(4):
            y_copy(c, m).start()

    def pass_on(c):
        for m, yy, xx in ((0, y_left, 0), (1, y_right, 1)):
            y_copy(c, m).wait_recv()
            where = rows_of(yy, xx)
            total = delta[c, where, :].astype(jnp.float32) + y_recv[c, m].astype(jnp.float32)
            delta[c, where, :] = total.astype(jnp.bfloat16)
            y_copy(c, m + 4).start()

    def sum_y(c):
        for m in (2, 3, 4, 5):
            y_copy(c, m).wait_recv()
        for xx, first, second in ((0, 3, 4), (1, 2, 5)):
            x_data[c, xx] = (
                delta[c, rows_of(y, xx), :].astype(jnp.float32)
                + y_recv[c, first].astype(jnp.float32)
                + y_recv[c, second].astype(jnp.float32)
            )
        x_copy(c).start()

    def sum_x(c):
        x_copy(c).wait_recv()
        for k in range(NZ):
            part = pl.ds(k * own, own)
            z_data[c, k] = x_data[c, x, part, :] + x_recv[c, part, :]
        for m in (3, 2, 1, 0, 6, 5, 4, 9, 10, 11, 12, 13, 14):
            z_copy(c, m).start()

    def pass_on_z(c):
        for m in range(7):
            z_copy(c, m).wait_recv()
        low = z_data[c, z_off(-4)] + z_recv[c, 0] + z_recv[c, 1]
        z_mid[c, 0] = low + z_recv[c, 2] + z_recv[c, 3]
        z_copy(c, 7).start()
        z_mid[c, 1] = z_data[c, z_off(4)] + z_recv[c, 4] + z_recv[c, 5] + z_recv[c, 6]
        z_copy(c, 8).start()

    def finish(c):
        for m in range(7, 15):
            z_copy(c, m).wait_recv()
        total = z_data[c, z]
        for m in range(7, 15):
            total = total + z_recv[c, m]
        where = pl.ds(pl.multiple_of(c * width, 128), width)
        total = prev_ref[:, where] + total
        aggregate_ref[:, where] = total
        squares[...] += total * total

    compute(0)
    pl.semaphore_wait(barrier, len(peers))

    @pl.loop(0, CHUNKS + 5)
    def _(s):
        @pl.when(s < CHUNKS)
        def _():
            @pl.when(s > 0)
            def _():
                compute(s)

            send_first(s)

        for lag, stage in enumerate((pass_on, sum_y, sum_x, pass_on_z, finish), 1):

            @pl.when((s >= lag) & (s < CHUNKS + lag))
            def _(lag=lag, stage=stage):
                stage(s - lag)

    sums_ref[0] = jnp.sum(squares[...])
    sums_ref[1] = jnp.sum(trigger_ref[...].astype(jnp.float32))

    @pl.loop(0, CHUNKS)
    def _(c):
        for m in range(6):
            y_copy(c, m).wait_send()
        x_copy(c).wait_send()
        for m in range(15):
            z_copy(c, m).wait_send()


def local(hidden_acts, out_grad, token_ids, trigger, stale, aggregate_prev):
    tokens, rows = hidden_acts.shape[1:]
    cols = out_grad.shape[2]
    width = cols // CHUNKS
    half = rows // (NY * NX)
    own = aggregate_prev.shape[1]
    vmem = pl.BlockSpec(memory_space=pltpu.VMEM)
    aggregate, sums = pl.pallas_call(
        functools.partial(reduce_kernel, rows, cols),
        out_shape=(
            jax.ShapeDtypeStruct((own, cols), jnp.float32),
            jax.ShapeDtypeStruct((2,), jnp.float32),
        ),
        in_specs=[vmem] * 5 + [pl.BlockSpec(memory_space=pl.ANY)],
        out_specs=(vmem, pl.BlockSpec(memory_space=pltpu.SMEM)),
        scratch_shapes=[
            pltpu.VMEM((rows, tokens), jnp.bfloat16),
            pltpu.VMEM((CHUNKS, tokens, width), jnp.bfloat16),
            pltpu.VMEM((rows // BLOCK, width), jnp.float32),
            pltpu.VMEM((CHUNKS, rows, width), jnp.bfloat16),
            pltpu.VMEM((CHUNKS, 6, half, width), jnp.bfloat16),
            pltpu.VMEM((CHUNKS, NX, half, width), jnp.float32),
            pltpu.VMEM((CHUNKS, half, width), jnp.float32),
            pltpu.VMEM((CHUNKS, NZ, own, width), jnp.float32),
            pltpu.VMEM((CHUNKS, 2, own, width), jnp.float32),
            pltpu.VMEM((CHUNKS, 15, own, width), jnp.float32),
            pltpu.VMEM((own, width), jnp.float32),
            pltpu.SemaphoreType.DMA((CHUNKS,)),
            pltpu.SemaphoreType.DMA((CHUNKS, 6)),
            pltpu.SemaphoreType.DMA((CHUNKS, 6)),
            pltpu.SemaphoreType.DMA((CHUNKS,)),
            pltpu.SemaphoreType.DMA((CHUNKS,)),
            pltpu.SemaphoreType.DMA((CHUNKS, 15)),
            pltpu.SemaphoreType.DMA((CHUNKS, 15)),
        ],
        compiler_params=pltpu.CompilerParams(
            collective_id=0, has_side_effects=True, vmem_limit_bytes=48 * 1024 * 1024
        ),
        name="reduce_deltas",
    )(hidden_acts[0], out_grad[0], token_ids, trigger, aggregate_prev[0], stale[0])
    square_total, triggered = lax.psum((sums[0], sums[1]), ("dp", "shard"))
    limit = clip_ratio * jnp.sqrt(jnp.asarray(4 * rows * cols, jnp.float32))
    clip_factor = jnp.minimum(1.0, limit / jnp.sqrt(square_total + epsilon))
    return (aggregate[None], (aggregate * clip_factor)[None], triggered)


def solution(mesh):
    in_specs = (
        P("dp", None, "shard"),
        P("dp", None, None),
        P("dp", None),
        P("dp", "shard"),
        P("dp", "shard", None),
        P("shard", "dp", None),
    )
    out_specs = (P("shard", "dp", None), P("shard", "dp", None), P())
    return jax.shard_map(local, mesh=mesh, in_specs=in_specs, out_specs=out_specs, check_vma=False)
```

```python
import functools

import jax
import jax.numpy as jnp
from jax import lax
from jax.experimental import pallas as pl
from jax.experimental.pallas import tpu as pltpu
from jax.sharding import PartitionSpec as P

BLOCK = 16
NY, NX, NZ = 4, 2, 16
NG = 2 * NX
CHUNKS = 8
MESH = pl.DeviceIdType.MESH

clip_ratio = 0.25
epsilon = 1e-06


def reduce_kernel(
    rows, cols,
    ids_hbm, trigger_hbm, grad_hbm, hidden_hbm, prev_hbm, stale_hbm,
    total_ref, factor_ref, count_ref,
    ids_ref, trigger_ref, grad_ref, hidden_ref, prev_ref,
    hidden_t, masked, keep, flags, delta, y_recv, x_data, x_recv, z_data, z_mid, z_recv, squares,
    n_data, n_recv_z, n_recv_p,
    input_sem, stale_sem, y_send_sem, y_recv_sem, x_send_sem, x_recv_sem, z_send_sem, z_recv_sem,
    n_send_sem, n_recv_sem,
):
    tokens = hidden_ref.shape[0]
    width = cols // CHUNKS
    half = rows // (NY * NX)
    own = half // NZ
    me = lax.axis_index("dp")
    shard = lax.axis_index("shard")
    y = me // (NX * NZ)
    x = (me // NZ) % NX
    z = me % NZ
    core = shard % 2
    group_x = (shard // 2) * NX + x
    y_right, y_left, y_far = (y + 1) % NY, (y + NY - 1) % NY, (y + 2) % NY

    def at(yy, xx, zz):
        return {"dp": yy * (NX * NZ) + xx * NZ + zz}

    right, left = at(y_right, x, z), at(y_left, x, z)
    across = at(y, 1 - x, z)

    def z_off(k):
        return (z + NZ + k) % NZ

    plane = [(oy, ox, oc) for oy in range(NY) for ox in range(NG) for oc in range(2)][1:]

    far_first = sorted(
        range(len(plane)), key=lambda i: -(min(plane[i][0], NY - plane[i][0]) + min(plane[i][1], NG - plane[i][1]))
    )

    def plane_peer(oy, ox, oc):
        yy, xx, cc = (y + oy) % NY, (group_x + ox) % NG, (core + oc) % 2
        return {"dp": yy * (NX * NZ) + (xx % NX) * NZ + z, "shard": (xx // NX) * 2 + cc}

    inputs = [
        pltpu.make_async_copy(source, target, input_sem.at[i])
        for i, (source, target) in enumerate((
            (ids_hbm, ids_ref), (trigger_hbm, trigger_ref), (grad_hbm, grad_ref),
            (hidden_hbm, hidden_ref), (prev_hbm, prev_ref),
        ))
    ]

    def stale_copy(c):
        return pltpu.make_async_copy(
            stale_hbm.at[:, pl.ds(pl.multiple_of(c * width, 128), width)],
            delta.at[c], stale_sem.at[c],
        )

    for copy in inputs[:4]:
        copy.start()
    for c in range(CHUNKS):
        stale_copy(c).start()
    inputs[4].start()

    barrier = pltpu.get_barrier_semaphore()
    for k in range(1, NZ):
        pl.semaphore_signal(barrier, inc=1, device_id=at(y, x, z_off(k)), device_id_type=MESH)
    for offset in plane:
        pl.semaphore_signal(barrier, inc=1, device_id=plane_peer(*offset), device_id_type=MESH)

    inputs[0].wait()
    inputs[1].wait()
    real = jnp.broadcast_to(ids_ref[...], (tokens, tokens)).T != 0
    real = jnp.where(real, 1.0, 0.0)
    blocks = rows // BLOCK
    sent = jnp.broadcast_to(trigger_ref[...].astype(jnp.float32), (blocks, blocks)).T
    for j in range(width // 128):
        keep[:, j * 128 : (j + 1) * 128] = real
        flags[:, j * 128 : (j + 1) * 128] = sent
    squares[...] = jnp.zeros_like(squares)

    def first_row(yy, xx):
        return pl.multiple_of(yy * (NX * half) + xx * half, half)

    def rows_of(yy, xx):
        return pl.ds(first_row(yy, xx), half)

    def y_copy(c, m):
        yy, xx, device = (
            (y_far, 0, left), (y_far, 1, right),
            (y_left, 1, left), (y_right, 0, right),
            (y_left, 0, left), (y_right, 1, right),
        )[m]
        return pltpu.make_async_remote_copy(
            delta.at[c, rows_of(yy, xx)], y_recv.at[c, m], y_send_sem.at[0], y_recv_sem.at[c, min(m, 2)],
            device_id=device, device_id_type=MESH,
        )

    def x_copy(c):
        return pltpu.make_async_remote_copy(
            x_data.at[c, 1 - x], x_recv.at[c], x_send_sem.at[0], x_recv_sem.at[c],
            device_id=across, device_id_type=MESH,
        )

    def z_copy(c, m):
        if m < 4:
            source, to = z_data.at[c, z_off(-(m + 5))], -(m + 1)
        elif m < 7:
            source, to = z_data.at[c, z_off(m + 1)], m - 3
        elif m < 9:
            source, to = z_mid.at[c, m - 7], (-4, 4)[m - 7]
        elif m < 12:
            source, to = z_data.at[c, z_off(-(m - 8))], -(m - 8)
        else:
            source, to = z_data.at[c, z_off(m - 11)], m - 11
        return pltpu.make_async_remote_copy(
            source, z_recv.at[c, m], z_send_sem.at[0], z_recv_sem.at[c, 0 if m < 7 else 1],
            device_id=at(y, x, z_off(to)), device_id_type=MESH,
        )

    def arrived(ref, sem):
        pltpu.make_async_copy(ref, ref, sem).wait()

    def compute(c, yy, xx, first):
        start = first_row(yy, xx)
        if first:
            for j in range(half // 128):
                part = pl.ds(pl.multiple_of(start + j * 128, 128), 128)
                hidden_t[part, :] = hidden_ref[:, part].T
        gradient = jnp.dot(
            hidden_t[pl.ds(start, half), :], masked[...], preferred_element_type=jnp.float32
        )
        diff = gradient - delta[c, pl.ds(start, half), :].astype(jnp.float32)
        for i in range(half // BLOCK):
            flag = flags[pl.ds(start // BLOCK + i, 1), :]
            delta[c, pl.ds(start + i * BLOCK, BLOCK), :] = (
                flag * diff[i * BLOCK : (i + 1) * BLOCK]
            ).astype(jnp.bfloat16)

    def begin(c, first=False):
        part = grad_ref[:, pl.ds(pl.multiple_of(c * width, 128), width)]
        masked[...] = (part.astype(jnp.float32) * keep[...]).astype(jnp.bfloat16)
        stale_copy(c).wait()
        compute(c, y_far, 0, first)
        compute(c, y_far, 1, first)
        if first:
            pl.semaphore_wait(barrier, NZ - 1 + len(plane))
        y_copy(c, 0).start()
        compute(c, y_left, 1, first)
        y_copy(c, 1).start()
        compute(c, y_right, 0, first)
        y_copy(c, 2).start()
        compute(c, y_left, 0, first)
        y_copy(c, 3).start()
        compute(c, y_right, 1, first)
        compute(c, y, 0, first)
        compute(c, y, 1, first)

    def pass_on(c):
        for m, yy, xx in ((0, y_left, 0), (1, y_right, 1)):
            y_copy(c, m).wait_recv()
            where = rows_of(yy, xx)
            total = delta[c, where, :].astype(jnp.float32) + y_recv[c, m].astype(jnp.float32)
            delta[c, where, :] = total.astype(jnp.bfloat16)
            y_copy(c, m + 4).start()

    def sum_y(c):
        arrived(y_recv.at[c, pl.ds(2, 4)], y_recv_sem.at[c, 2])
        for xx, first, second in ((0, 3, 4), (1, 2, 5)):
            x_data[c, xx] = (
                delta[c, rows_of(y, xx), :].astype(jnp.float32)
                + y_recv[c, first].astype(jnp.float32)
                + y_recv[c, second].astype(jnp.float32)
            )
        x_copy(c).start()

    def sum_x(c):
        x_copy(c).wait_recv()
        for k in range(NZ):
            part = pl.ds(k * own, own)
            z_data[c, k] = x_data[c, x, part, :] + x_recv[c, part, :]
        for m in (3, 2, 1, 0, 6, 5, 4, 11, 10, 9, 14, 13, 12):
            z_copy(c, m).start()

    def pass_on_z(c):
        arrived(z_recv.at[c, pl.ds(0, 7)], z_recv_sem.at[c, 0])
        low = z_data[c, z_off(-4)] + z_recv[c, 0] + z_recv[c, 1]
        z_mid[c, 0] = low + z_recv[c, 2] + z_recv[c, 3]
        z_copy(c, 7).start()
        z_mid[c, 1] = z_data[c, z_off(4)] + z_recv[c, 4] + z_recv[c, 5] + z_recv[c, 6]
        z_copy(c, 8).start()

    def finish(c):
        arrived(z_recv.at[c, pl.ds(7, 8)], z_recv_sem.at[c, 1])
        total = z_data[c, z]
        for m in range(7, 15):
            total = total + z_recv[c, m]
        where = pl.ds(pl.multiple_of(c * width, 128), width)
        total_ref[:, where] = total
        total = prev_ref[:, where] + total
        squares[...] += total * total

    inputs[2].wait()
    inputs[3].wait()
    begin(0, first=True)

    @pl.loop(1, CHUNKS + 5)
    def _(s):
        @pl.when(s < CHUNKS)
        def _():
            begin(s)

        @pl.when(s == 1)
        def _():
            inputs[4].wait()

        for lag, stage in enumerate((pass_on, sum_y, sum_x, pass_on_z, finish), 1):

            @pl.when((s >= lag) & (s < CHUNKS + lag))
            def _(lag=lag, stage=stage):
                stage(s - lag)

    lanes = squares[0:8, 0:128]
    for i in range(own // 8):
        for j in range(width // 128):
            if i + j > 0:
                lanes = lanes + squares[i * 8 : (i + 1) * 8, j * 128 : (j + 1) * 128]
    lanes = jnp.sum(lanes, axis=0, keepdims=True)
    n_data[0, 0:1, :] = lanes
    n_data[0, 1:2, :] = trigger_ref[...].astype(jnp.float32)

    def n_copy(k):
        return pltpu.make_async_remote_copy(
            n_data.at[0], n_recv_z.at[k - 1], n_send_sem.at[0], n_recv_sem.at[0],
            device_id=at(y, x, z_off(k)), device_id_type=MESH,
        )

    def p_copy(i):
        return pltpu.make_async_remote_copy(
            n_data.at[1], n_recv_p.at[i], n_send_sem.at[1], n_recv_sem.at[1],
            device_id=plane_peer(*plane[i]), device_id_type=MESH,
        )

    for k in (8, 7, 9, 6, 10, 5, 11, 4, 12, 3, 13, 2, 14, 1, 15):
        n_copy(k).start()
    arrived(y_recv, y_send_sem.at[0])
    arrived(x_recv, x_send_sem.at[0])
    arrived(z_recv, z_send_sem.at[0])
    arrived(n_recv_z, n_recv_sem.at[0])
    n_data[1] = n_data[0] + jnp.sum(n_recv_z[...], axis=0)
    for i in far_first:
        p_copy(i).start()
    arrived(n_recv_z, n_send_sem.at[0])
    arrived(n_recv_p, n_recv_sem.at[1])
    both = n_data[1] + jnp.sum(n_recv_p[...], axis=0)
    square_total = jnp.sum(both[0:1, :], axis=1, keepdims=True)
    limit = clip_ratio * jnp.sqrt(jnp.full((1, 1), 4 * rows * cols, jnp.float32))
    factor_ref[...] = jnp.minimum(1.0, limit / jnp.sqrt(square_total + epsilon))
    count_ref[...] = jnp.sum(both[1:2, :], axis=1, keepdims=True)

    arrived(n_recv_p, n_send_sem.at[1])


def local(hidden_acts, out_grad, token_ids, trigger, stale, aggregate_prev):
    tokens, rows = hidden_acts.shape[1:]
    cols = out_grad.shape[2]
    width = cols // CHUNKS
    half = rows // (NY * NX)
    own = aggregate_prev.shape[1]
    vmem = pl.BlockSpec(memory_space=pltpu.VMEM)
    hbm = pl.BlockSpec(memory_space=pltpu.HBM)
    bf16, f32 = jnp.bfloat16, jnp.float32
    dma = pltpu.SemaphoreType.DMA
    total, factor, count = pl.pallas_call(
        functools.partial(reduce_kernel, rows, cols),
        out_shape=(
            jax.ShapeDtypeStruct((own, cols), f32),
            jax.ShapeDtypeStruct((1, 1), f32),
            jax.ShapeDtypeStruct((1, 1), f32),
        ),
        in_specs=[hbm] * 6,
        out_specs=(vmem,) * 3,
        scratch_shapes=[
            pltpu.VMEM(token_ids.shape, jnp.int32),
            pltpu.VMEM(trigger.shape, jnp.int32),
            pltpu.VMEM((tokens, cols), bf16),
            pltpu.VMEM((tokens, rows), bf16),
            pltpu.VMEM((own, cols), f32),
            pltpu.VMEM((rows, tokens), bf16),
            pltpu.VMEM((tokens, width), bf16),
            pltpu.VMEM((tokens, width), f32),
            pltpu.VMEM((rows // BLOCK, width), f32),
            pltpu.VMEM((CHUNKS, rows, width), bf16),
            pltpu.VMEM((CHUNKS, 6, half, width), bf16),
            pltpu.VMEM((CHUNKS, NX, half, width), f32),
            pltpu.VMEM((CHUNKS, half, width), f32),
            pltpu.VMEM((CHUNKS, NZ, own, width), f32),
            pltpu.VMEM((CHUNKS, 2, own, width), f32),
            pltpu.VMEM((CHUNKS, 15, own, width), f32),
            pltpu.VMEM((own, width), f32),
            pltpu.VMEM((2, 2, 128), f32),
            pltpu.VMEM((NZ - 1, 2, 128), f32),
            pltpu.VMEM((NY * NG * 2 - 1, 2, 128), f32),
            dma((5,)),
            dma((CHUNKS,)),
            dma((1,)),
            dma((CHUNKS, 3)),
            dma((1,)),
            dma((CHUNKS,)),
            dma((1,)),
            dma((CHUNKS, 2)),
            dma((2,)),
            dma((2,)),
        ],
        compiler_params=pltpu.CompilerParams(
            collective_id=0, has_side_effects=True, vmem_limit_bytes=67_000_000
        ),
        name="reduce_deltas",
    )(token_ids, trigger, out_grad[0], hidden_acts[0], aggregate_prev[0], stale[0])
    aggregate = aggregate_prev[0] + total
    return (aggregate[None], (aggregate * factor)[None], count[0, 0])


def solution(mesh):
    in_specs = (
        P("dp", None, "shard"),
        P("dp", None, None),
        P("dp", None),
        P("dp", "shard"),
        P("dp", "shard", None),
        P("shard", "dp", None),
    )
    out_specs = (P("shard", "dp", None), P("shard", "dp", None), P())
    return jax.shard_map(local, mesh=mesh, in_specs=in_specs, out_specs=out_specs, check_vma=False)
```

```python
import functools

import jax
import jax.numpy as jnp
from jax import lax
from jax.experimental import pallas as pl
from jax.experimental.pallas import tpu as pltpu
from jax.sharding import PartitionSpec as P

BLOCK = 16
NY, NX, NZ = 4, 2, 16
NG = 2 * NX
CHUNKS = 8
MESH = pl.DeviceIdType.MESH

clip_ratio = 0.25
epsilon = 1e-06


def reduce_kernel(
    rows, cols,
    ids_hbm, trigger_hbm, grad_hbm, hidden_hbm, prev_hbm, stale_hbm,
    total_hbm, factor_ref, count_ref,
    ids_ref, trigger_ref, grad_ref, hidden_ref, prev_ref,
    total_ref, hidden_t, masked, keep, flags, delta, y_recv, x_data, x_recv, z_data, z_mid, z_recv, squares,
    n_data, n_recv_z, n_recv_p,
    input_sem, stale_sem, y_send_sem, y_recv_sem, x_send_sem, x_recv_sem, z_send_sem, z_recv_sem,
    n_send_sem, n_recv_sem, word_sem,
):
    tokens = hidden_ref.shape[0]
    width = cols // CHUNKS
    half = rows // (NY * NX)
    own = half // NZ
    me = lax.axis_index("dp")
    shard = lax.axis_index("shard")
    y = me // (NX * NZ)
    x = (me // NZ) % NX
    z = me % NZ
    core = shard % 2
    group_x = (shard // 2) * NX + x
    y_right, y_left, y_far = (y + 1) % NY, (y + NY - 1) % NY, (y + 2) % NY

    def at(yy, xx, zz):
        return {"dp": yy * (NX * NZ) + xx * NZ + zz}

    right, left = at(y_right, x, z), at(y_left, x, z)
    across = at(y, 1 - x, z)

    def z_off(k):
        return (z + NZ + k) % NZ

    plane = [(oy, ox, oc) for oy in range(NY) for ox in range(NG) for oc in range(2)][1:]

    far_first = sorted(
        range(len(plane)), key=lambda i: -(min(plane[i][0], NY - plane[i][0]) + min(plane[i][1], NG - plane[i][1]))
    )

    def plane_peer(oy, ox, oc):
        yy, xx, cc = (y + oy) % NY, (group_x + ox) % NG, (core + oc) % 2
        return {"dp": yy * (NX * NZ) + (xx % NX) * NZ + z, "shard": (xx // NX) * 2 + cc}

    moves = [
        pltpu.make_async_copy(source, target, input_sem.at[i])
        for i, (source, target) in enumerate((
            (ids_hbm, ids_ref), (trigger_hbm, trigger_ref), (grad_hbm, grad_ref),
            (hidden_hbm, hidden_ref), (prev_hbm, prev_ref), (total_ref, total_hbm),
        ))
    ]

    def stale_copy(c):
        return pltpu.make_async_copy(
            stale_hbm.at[:, pl.ds(pl.multiple_of(c * width, 128), width)],
            delta.at[c], stale_sem.at[c],
        )

    for copy in moves[:4]:
        copy.start()
    stale_copy(0).start()
    stale_copy(1).start()

    barrier = pltpu.get_barrier_semaphore()
    near = [right, left, across, at(y, x, z_off(1)), at(y, x, z_off(-1))]
    near += [plane_peer(0, 0, 1), plane_peer(0, NX, 0), plane_peer(0, NX, 1)]
    for peer in near:
        pl.semaphore_signal(barrier, inc=1, device_id=peer, device_id_type=MESH)

    def tell_z(i):
        for k in (1, -1):
            pl.semaphore_signal(word_sem.at[i], inc=1, device_id=at(y, x, z_off(k)), device_id_type=MESH)

    moves[0].wait()
    moves[1].wait()
    real = jnp.broadcast_to(ids_ref[...], (tokens, tokens)).T != 0
    real = jnp.where(real, 1.0, 0.0)
    blocks = rows // BLOCK
    sent = jnp.broadcast_to(trigger_ref[...].astype(jnp.float32), (blocks, blocks)).T
    for j in range(width // 128):
        keep[:, j * 128 : (j + 1) * 128] = real
        flags[:, j * 128 : (j + 1) * 128] = sent
    squares[...] = jnp.zeros_like(squares)

    def first_row(yy, xx):
        return pl.multiple_of(yy * (NX * half) + xx * half, half)

    def rows_of(yy, xx):
        return pl.ds(first_row(yy, xx), half)

    def y_copy(c, m):
        yy, xx, device = (
            (y_far, 0, left), (y_far, 1, right),
            (y_left, 1, left), (y_right, 0, right),
            (y_left, 0, left), (y_right, 1, right),
        )[m]
        return pltpu.make_async_remote_copy(
            delta.at[c, rows_of(yy, xx)], y_recv.at[c, m], y_send_sem.at[0], y_recv_sem.at[c, min(m, 2)],
            device_id=device, device_id_type=MESH,
        )

    def x_copy(c):
        return pltpu.make_async_remote_copy(
            x_data.at[c, 1 - x], x_recv.at[c], x_send_sem.at[0], x_recv_sem.at[c],
            device_id=across, device_id_type=MESH,
        )

    def z_copy(c, m):
        if m < 4:
            source, to = z_data.at[c, z_off(-(m + 5))], -(m + 1)
        elif m < 7:
            source, to = z_data.at[c, z_off(m + 1)], m - 3
        elif m < 9:
            source, to = z_mid.at[c, m - 7], (-4, 4)[m - 7]
        elif m < 12:
            source, to = z_data.at[c, z_off(-(m - 8))], -(m - 8)
        else:
            source, to = z_data.at[c, z_off(m - 11)], m - 11
        return pltpu.make_async_remote_copy(
            source, z_recv.at[c, m], z_send_sem.at[0], z_recv_sem.at[c, 0 if m < 7 else 1],
            device_id=at(y, x, z_off(to)), device_id_type=MESH,
        )

    def arrived(ref, sem):
        pltpu.make_async_copy(ref, ref, sem).wait()

    def compute(c, yy, xx, first):
        start = first_row(yy, xx)
        if first:
            for j in range(half // 128):
                part = pl.ds(pl.multiple_of(start + j * 128, 128), 128)
                hidden_t[part, :] = hidden_ref[:, part].T
        gradient = jnp.dot(
            hidden_t[pl.ds(start, half), :], masked[...], preferred_element_type=jnp.float32
        )
        diff = gradient - delta[c, pl.ds(start, half), :].astype(jnp.float32)
        for i in range(half // BLOCK):
            flag = flags[pl.ds(start // BLOCK + i, 1), :]
            delta[c, pl.ds(start + i * BLOCK, BLOCK), :] = (
                flag * diff[i * BLOCK : (i + 1) * BLOCK]
            ).astype(jnp.bfloat16)

    def begin(c, first=False):
        part = grad_ref[:, pl.ds(pl.multiple_of(c * width, 128), width)]
        masked[...] = (part.astype(jnp.float32) * keep[...]).astype(jnp.bfloat16)
        stale_copy(c).wait()

        @pl.when(c + 2 < CHUNKS)
        def _():
            stale_copy(c + 2).start()

        compute(c, y_far, 0, first)
        compute(c, y_far, 1, first)
        if first:
            pl.semaphore_wait(barrier, len(near))
            tell_z(0)
        y_copy(c, 0).start()
        compute(c, y_left, 1, first)
        y_copy(c, 1).start()
        compute(c, y_right, 0, first)
        y_copy(c, 2).start()
        compute(c, y_left, 0, first)
        y_copy(c, 3).start()
        compute(c, y_right, 1, first)
        compute(c, y, 0, first)
        compute(c, y, 1, first)

    def pass_on(c):
        for m, yy, xx in ((0, y_left, 0), (1, y_right, 1)):
            y_copy(c, m).wait_recv()
            where = rows_of(yy, xx)
            total = delta[c, where, :].astype(jnp.float32) + y_recv[c, m].astype(jnp.float32)
            delta[c, where, :] = total.astype(jnp.bfloat16)
            y_copy(c, m + 4).start()

    def sum_y(c):
        arrived(y_recv.at[c, pl.ds(2, 4)], y_recv_sem.at[c, 2])
        for xx, first, second in ((0, 3, 4), (1, 2, 5)):
            x_data[c, xx] = (
                delta[c, rows_of(y, xx), :].astype(jnp.float32)
                + y_recv[c, first].astype(jnp.float32)
                + y_recv[c, second].astype(jnp.float32)
            )
        x_copy(c).start()

    def sum_x(c):
        x_copy(c).wait_recv()
        for k in range(NZ):
            part = pl.ds(k * own, own)
            z_data[c, k] = x_data[c, x, part, :] + x_recv[c, part, :]
        for m in (3, 2, 1, 0, 6, 5, 4, 11, 10, 9, 14, 13, 12):
            z_copy(c, m).start()

    def pass_on_z(c):
        arrived(z_recv.at[c, pl.ds(0, 7)], z_recv_sem.at[c, 0])
        low = z_data[c, z_off(-4)] + z_recv[c, 0] + z_recv[c, 1]
        z_mid[c, 0] = low + z_recv[c, 2] + z_recv[c, 3]
        z_copy(c, 7).start()
        z_mid[c, 1] = z_data[c, z_off(4)] + z_recv[c, 4] + z_recv[c, 5] + z_recv[c, 6]
        z_copy(c, 8).start()

    def finish(c):
        arrived(z_recv.at[c, pl.ds(7, 8)], z_recv_sem.at[c, 1])
        total = z_data[c, z]
        for m in range(7, 15):
            total = total + z_recv[c, m]
        where = pl.ds(pl.multiple_of(c * width, 128), width)
        total_ref[:, where] = total
        total = prev_ref[:, where] + total
        squares[...] += total * total

    moves[2].wait()
    moves[3].wait()
    begin(0, first=True)
    moves[4].start()

    @pl.loop(1, CHUNKS + 5)
    def _(s):
        @pl.when(s < CHUNKS)
        def _():
            begin(s)

        for i in range(3):

            @pl.when(s == i + 1)
            def _(i=i):
                pl.semaphore_wait(word_sem.at[i], 2)
                if i < 2:
                    tell_z(i + 1)
                else:
                    moves[4].wait()

        for lag, stage in enumerate((pass_on, sum_y, sum_x, pass_on_z, finish), 1):

            @pl.when((s >= lag) & (s < CHUNKS + lag))
            def _(lag=lag, stage=stage):
                stage(s - lag)

    lanes = squares[0:8, 0:128]
    for i in range(own // 8):
        for j in range(width // 128):
            if i + j > 0:
                lanes = lanes + squares[i * 8 : (i + 1) * 8, j * 128 : (j + 1) * 128]
    lanes = jnp.sum(lanes, axis=0, keepdims=True)
    n_data[0, 0:1, :] = lanes
    n_data[0, 1:2, :] = trigger_ref[...].astype(jnp.float32)

    def n_copy(k):
        return pltpu.make_async_remote_copy(
            n_data.at[0], n_recv_z.at[k - 1], n_send_sem.at[0], n_recv_sem.at[0],
            device_id=at(y, x, z_off(k)), device_id_type=MESH,
        )

    def p_copy(i):
        return pltpu.make_async_remote_copy(
            n_data.at[1], n_recv_p.at[i], n_send_sem.at[1], n_recv_sem.at[1],
            device_id=plane_peer(*plane[i]), device_id_type=MESH,
        )

    for k in (8, 7, 9, 6, 10, 5, 11, 4, 12, 3, 13, 2, 14, 1, 15):
        n_copy(k).start()
    moves[5].start()
    arrived(y_recv, y_send_sem.at[0])
    arrived(x_recv, x_send_sem.at[0])
    arrived(z_recv, z_send_sem.at[0])
    arrived(n_recv_z, n_recv_sem.at[0])
    n_data[1] = n_data[0] + jnp.sum(n_recv_z[...], axis=0)
    for i in far_first:
        p_copy(i).start()
    arrived(n_recv_z, n_send_sem.at[0])
    moves[5].wait()
    arrived(n_recv_p, n_recv_sem.at[1])
    both = n_data[1] + jnp.sum(n_recv_p[...], axis=0)
    square_total = jnp.sum(both[0:1, :], axis=1, keepdims=True)
    limit = clip_ratio * jnp.sqrt(jnp.full((1, 1), 4 * rows * cols, jnp.float32))
    factor_ref[...] = jnp.minimum(1.0, limit / jnp.sqrt(square_total + epsilon))
    count_ref[...] = jnp.sum(both[1:2, :], axis=1, keepdims=True)

    arrived(n_recv_p, n_send_sem.at[1])


def local(hidden_acts, out_grad, token_ids, trigger, stale, aggregate_prev):
    tokens, rows = hidden_acts.shape[1:]
    cols = out_grad.shape[2]
    width = cols // CHUNKS
    half = rows // (NY * NX)
    own = aggregate_prev.shape[1]
    vmem = pl.BlockSpec(memory_space=pltpu.VMEM)
    hbm = pl.BlockSpec(memory_space=pltpu.HBM)
    bf16, f32 = jnp.bfloat16, jnp.float32
    dma = pltpu.SemaphoreType.DMA
    total, factor, count = pl.pallas_call(
        functools.partial(reduce_kernel, rows, cols),
        out_shape=(
            jax.ShapeDtypeStruct((own, cols), f32),
            jax.ShapeDtypeStruct((1, 1), f32),
            jax.ShapeDtypeStruct((1, 1), f32),
        ),
        in_specs=[hbm] * 6,
        out_specs=(hbm, vmem, vmem),
        scratch_shapes=[
            pltpu.VMEM(token_ids.shape, jnp.int32),
            pltpu.VMEM(trigger.shape, jnp.int32),
            pltpu.VMEM((tokens, cols), bf16),
            pltpu.VMEM((tokens, rows), bf16),
            pltpu.VMEM((own, cols), f32),
            pltpu.VMEM((own, cols), f32),
            pltpu.VMEM((rows, tokens), bf16),
            pltpu.VMEM((tokens, width), bf16),
            pltpu.VMEM((tokens, width), f32),
            pltpu.VMEM((rows // BLOCK, width), f32),
            pltpu.VMEM((CHUNKS, rows, width), bf16),
            pltpu.VMEM((CHUNKS, 6, half, width), bf16),
            pltpu.VMEM((CHUNKS, NX, half, width), f32),
            pltpu.VMEM((CHUNKS, half, width), f32),
            pltpu.VMEM((CHUNKS, NZ, own, width), f32),
            pltpu.VMEM((CHUNKS, 2, own, width), f32),
            pltpu.VMEM((CHUNKS, 15, own, width), f32),
            pltpu.VMEM((own, width), f32),
            pltpu.VMEM((2, 2, 128), f32),
            pltpu.VMEM((NZ - 1, 2, 128), f32),
            pltpu.VMEM((NY * NG * 2 - 1, 2, 128), f32),
            dma((6,)),
            dma((CHUNKS,)),
            dma((1,)),
            dma((CHUNKS, 3)),
            dma((1,)),
            dma((CHUNKS,)),
            dma((1,)),
            dma((CHUNKS, 2)),
            dma((2,)),
            dma((2,)),
            pltpu.SemaphoreType.REGULAR((3,)),
        ],
        compiler_params=pltpu.CompilerParams(
            collective_id=0, has_side_effects=True, vmem_limit_bytes=66_900_000
        ),
        name="reduce_deltas",
    )(token_ids, trigger, out_grad[0], hidden_acts[0], aggregate_prev[0], stale[0])
    aggregate = aggregate_prev[0] + total
    return (aggregate[None], (aggregate * factor)[None], count[0, 0])


def solution(mesh):
    in_specs = (
        P("dp", None, "shard"),
        P("dp", None, None),
        P("dp", None),
        P("dp", "shard"),
        P("dp", "shard", None),
        P("shard", "dp", None),
    )
    out_specs = (P("shard", "dp", None), P("shard", "dp", None), P())
    return jax.shard_map(local, mesh=mesh, in_specs=in_specs, out_specs=out_specs, check_vma=False)
```

```python
import functools

import jax
import jax.numpy as jnp
from jax import lax
from jax.experimental import pallas as pl
from jax.experimental.pallas import tpu as pltpu
from jax.sharding import PartitionSpec as P

BLOCK = 16
NY, NX, NZ = 4, 2, 16
NG = 2 * NX
CHUNKS = 8
EVERY = 4
X_FIRST = CHUNKS // EVERY
LEAD = 2
MESH = pl.DeviceIdType.MESH

clip_ratio = 0.25
epsilon = 1e-06


def reduce_kernel(
    rows, cols,
    ids_hbm, trigger_hbm, grad_hbm, hidden_hbm, prev_hbm, stale_hbm,
    total_hbm, factor_ref, count_ref,
    ids_ref, trigger_ref, grad_ref, hidden_ref, prev_ref,
    total_ref, hidden_t, masked, keep, flags, delta, y_recv, x_data, x_recv, pair_recv, z_data, z_mid, z_recv, squares,
    n_data, n_recv_z, n_recv_p,
    input_sem, stale_sem, y_send_sem, y_recv_sem, x_send_sem, x_recv_sem, pair_sem, z_send_sem, z_recv_sem,
    n_send_sem, n_recv_sem, word_sem,
):
    tokens = hidden_ref.shape[0]
    width = cols // CHUNKS
    half = rows // (NY * NX)
    own = half // NZ
    me = lax.axis_index("dp")
    shard = lax.axis_index("shard")
    y = me // (NX * NZ)
    x = (me // NZ) % NX
    z = me % NZ
    core = shard % 2
    group_x = (shard // 2) * NX + x
    y_right, y_left, y_far = (y + 1) % NY, (y + NY - 1) % NY, (y + 2) % NY

    def at(yy, xx, zz):
        return {"dp": yy * (NX * NZ) + xx * NZ + zz}

    right, left = at(y_right, x, z), at(y_left, x, z)
    across = at(y, 1 - x, z)

    def z_off(k):
        return (z + NZ + k) % NZ

    plane = [(oy, ox, oc) for oy in range(NY) for ox in range(NG) for oc in range(2)][1:]

    far_first = sorted(
        range(len(plane)), key=lambda i: -(min(plane[i][0], NY - plane[i][0]) + min(plane[i][1], NG - plane[i][1]))
    )

    def plane_peer(oy, ox, oc):
        yy, xx, cc = (y + oy) % NY, (group_x + ox) % NG, (core + oc) % 2
        return {"dp": yy * (NX * NZ) + (xx % NX) * NZ + z, "shard": (xx // NX) * 2 + cc}

    moves = [
        pltpu.make_async_copy(source, target, input_sem.at[i])
        for i, (source, target) in enumerate((
            (ids_hbm, ids_ref), (trigger_hbm, trigger_ref), (grad_hbm, grad_ref),
            (hidden_hbm, hidden_ref), (prev_hbm, prev_ref), (total_ref, total_hbm),
        ))
    ]

    def stale_copy(c):
        return pltpu.make_async_copy(
            stale_hbm.at[:, pl.ds(pl.multiple_of(c * width, 128), width)],
            delta.at[c], stale_sem.at[c],
        )

    for copy in moves[:4]:
        copy.start()
    for c in (0, EVERY - 1, 1):
        stale_copy(c).start()

    barrier = pltpu.get_barrier_semaphore()
    near = [right, left, across, at(y, x, z_off(1)), at(y, x, z_off(-1))]
    near += [plane_peer(0, 0, 1), plane_peer(0, NX, 0), plane_peer(0, NX, 1)]
    for peer in near:
        pl.semaphore_signal(barrier, inc=1, device_id=peer, device_id_type=MESH)

    def tell_z(i):
        for k in (1, -1):
            pl.semaphore_signal(word_sem.at[i], inc=1, device_id=at(y, x, z_off(k)), device_id_type=MESH)

    moves[0].wait()
    moves[1].wait()
    real = jnp.broadcast_to(ids_ref[...], (tokens, tokens)).T != 0
    real = jnp.where(real, 1.0, 0.0)
    blocks = rows // BLOCK
    sent = jnp.broadcast_to(trigger_ref[...].astype(jnp.float32), (blocks, blocks)).T
    for j in range(width // 128):
        keep[:, j * 128 : (j + 1) * 128] = real
        flags[:, j * 128 : (j + 1) * 128] = sent
    squares[...] = jnp.zeros_like(squares)

    def first_row(yy, xx):
        return pl.multiple_of(yy * (NX * half) + xx * half, half)

    def rows_of(yy, xx):
        return pl.ds(first_row(yy, xx), half)

    def y_copy(c, m):
        yy, xx, device = (
            (y_far, 0, left), (y_far, 1, right),
            (y_left, 1, left), (y_right, 0, right),
            (y_left, 0, left), (y_right, 1, right),
        )[m]
        return pltpu.make_async_remote_copy(
            delta.at[c, rows_of(yy, xx)], y_recv.at[c, m], y_send_sem.at[0], y_recv_sem.at[c, min(m, 2)],
            device_id=device, device_id_type=MESH,
        )

    def x_copy(c):
        return pltpu.make_async_remote_copy(
            x_data.at[c, 1 - x], x_recv.at[c], x_send_sem.at[0], x_recv_sem.at[c],
            device_id=across, device_id_type=MESH,
        )

    z_messages = (
        (-8, -2, 0, None), (-7, -1, 0, None), (7, 1, 0, None),
        (-5, -2, 1, None), (-4, -1, 1, None), (None, -3, 1, 0),
        (5, 2, 1, None), (4, 1, 1, None), (None, 3, 1, 1),
        (-2, -2, 2, None), (-1, -1, 2, None), (None, -3, 2, 2),
        (2, 2, 2, None), (1, 1, 2, None), (None, 3, 2, 3),
    )

    def z_copy(c, m):
        k, hops, batch, middle = z_messages[m]
        source = z_data.at[c, z_off(k)] if middle is None else z_mid.at[c, middle]
        return pltpu.make_async_remote_copy(
            source, z_recv.at[c, m], z_send_sem.at[0], z_recv_sem.at[c, batch],
            device_id=at(y, x, z_off(hops)), device_id_type=MESH,
        )

    def arrived(ref, sem):
        pltpu.make_async_copy(ref, ref, sem).wait()

    def compute(c, yy, xx, first):
        start = first_row(yy, xx)
        if first:
            for j in range(half // 128):
                part = pl.ds(pl.multiple_of(start + j * 128, 128), 128)
                hidden_t[part, :] = hidden_ref[:, part].T
        gradient = jnp.dot(
            hidden_t[pl.ds(start, half), :], masked[...], preferred_element_type=jnp.float32
        )
        diff = gradient - delta[c, pl.ds(start, half), :].astype(jnp.float32)
        for i in range(half // BLOCK):
            flag = flags[pl.ds(start // BLOCK + i, 1), :]
            delta[c, pl.ds(start + i * BLOCK, BLOCK), :] = (
                flag * diff[i * BLOCK : (i + 1) * BLOCK]
            ).astype(jnp.bfloat16)

    def prepare(c):
        part = grad_ref[:, pl.ds(pl.multiple_of(c * width, 128), width)]
        masked[...] = (part.astype(jnp.float32) * keep[...]).astype(jnp.bfloat16)
        stale_copy(c).wait()

    def begin(c, first=False):
        prepare(c)
        compute(c, y_far, 0, first)
        compute(c, y_far, 1, first)
        if first:
            pl.semaphore_wait(barrier, len(near))
            tell_z(0)
        y_copy(c, 0).start()
        compute(c, y_left, 1, first)
        y_copy(c, 1).start()
        compute(c, y_right, 0, first)
        y_copy(c, 2).start()
        compute(c, y_left, 0, first)
        y_copy(c, 3).start()
        compute(c, y_right, 1, first)
        compute(c, y, 0, first)
        compute(c, y, 1, first)

    def pass_on(c):
        for m, yy, xx in ((0, y_left, 0), (1, y_right, 1)):
            y_copy(c, m).wait_recv()
            where = rows_of(yy, xx)
            total = delta[c, where, :].astype(jnp.float32) + y_recv[c, m].astype(jnp.float32)
            delta[c, where, :] = total.astype(jnp.bfloat16)
            y_copy(c, m + 4).start()

    def sum_y(c):
        arrived(y_recv.at[c, pl.ds(2, 4)], y_recv_sem.at[c, 2])
        for xx, first, second in ((0, 3, 4), (1, 2, 5)):
            x_data[c, xx] = (
                delta[c, rows_of(y, xx), :].astype(jnp.float32)
                + y_recv[c, first].astype(jnp.float32)
                + y_recv[c, second].astype(jnp.float32)
            )
        x_copy(c).start()

    def pair_copy(c, yy):
        return pltpu.make_async_remote_copy(
            delta.at[c, rows_of(yy, 1 - x)], pair_recv.at[c // EVERY, yy],
            x_send_sem.at[1], pair_sem.at[c // EVERY],
            device_id=across, device_id_type=MESH,
        )

    quarter = half // 2

    def part_of(yy, h):
        return pl.ds(pl.multiple_of(first_row(yy, x) + h * quarter, quarter), quarter)

    def y_pair_copy(c, m):
        yy, h, device = (
            (y_far, 0, left), (y_far, 1, right),
            (y_left, 1, left), (y_right, 0, right),
            (y_left, 0, left), (y_right, 1, right),
        )[m]
        return pltpu.make_async_remote_copy(
            delta.at[c, part_of(yy, h)], y_recv.at[c, m, pl.ds(0, quarter)],
            y_send_sem.at[0], y_recv_sem.at[c, min(m, 2)],
            device_id=device, device_id_type=MESH,
        )

    def begin_pair(c):
        prepare(c)
        for yy in range(NY):
            compute(c, yy, 1 - x, False)
            if yy > 0:
                pair_copy(c, yy - 1).start()
        compute(c, 0, x, False)
        pair_copy(c, NY - 1).start()
        for yy in range(1, NY):
            compute(c, yy, x, False)

    def sum_pair(c):
        arrived(pair_recv.at[c // EVERY], pair_sem.at[c // EVERY])

        def both(yy):
            return delta[c, rows_of(yy, x), :].astype(jnp.float32) + pair_recv[c // EVERY, yy].astype(jnp.float32)

        for yy in (y_far, y_left, y_right):
            delta[c, rows_of(yy, x), :] = both(yy).astype(jnp.bfloat16)
        for m in range(4):
            y_pair_copy(c, m).start()
        x_data[c, 0] = both(y)

    def pass_on_pair(c):
        for m, yy, h in ((0, y_left, 0), (1, y_right, 1)):
            y_pair_copy(c, m).wait_recv()
            where = part_of(yy, h)
            total = delta[c, where, :].astype(jnp.float32) + y_recv[c, m, pl.ds(0, quarter), :].astype(jnp.float32)
            delta[c, where, :] = total.astype(jnp.bfloat16)
            y_pair_copy(c, m + 4).start()

    def send_z(c):
        for m in (0, 2, 1, 3, 6, 4, 7, 9, 12, 10, 13):
            z_copy(c, m).start()

    def sum_y_pair(c):
        arrived(y_recv.at[c, pl.ds(2, 2)], y_recv_sem.at[c, 2])
        for h, first, second in ((0, 3, 4), (1, 2, 5)):
            for k in range(NZ // 2):
                part = pl.ds(k * own, own)
                z_data[c, h * (NZ // 2) + k] = (
                    x_data[c, 0, pl.ds(h * quarter + k * own, own), :]
                    + y_recv[c, first, part, :].astype(jnp.float32)
                    + y_recv[c, second, part, :].astype(jnp.float32)
                )
        send_z(c)

    def sum_x(c):
        x_copy(c).wait_recv()
        for k in range(NZ):
            part = pl.ds(k * own, own)
            z_data[c, k] = x_data[c, x, part, :] + x_recv[c, part, :]
        send_z(c)

    def pass_on_z(c):
        arrived(z_recv.at[c, pl.ds(0, 3)], z_recv_sem.at[c, 0])
        z_mid[c, 0] = z_data[c, z_off(-6)] + z_recv[c, 0] + z_recv[c, 1]
        z_copy(c, 5).start()
        z_mid[c, 1] = z_data[c, z_off(6)] + z_recv[c, 2]
        z_copy(c, 8).start()

    def pass_on_again(c):
        arrived(z_recv.at[c, pl.ds(3, 6)], z_recv_sem.at[c, 1])
        z_mid[c, 2] = z_data[c, z_off(-3)] + z_recv[c, 3] + z_recv[c, 4] + z_recv[c, 5]
        z_copy(c, 11).start()
        z_mid[c, 3] = z_data[c, z_off(3)] + z_recv[c, 6] + z_recv[c, 7] + z_recv[c, 8]
        z_copy(c, 14).start()

    def finish(c):
        arrived(z_recv.at[c, pl.ds(9, 6)], z_recv_sem.at[c, 2])
        total = z_data[c, z]
        for m in range(9, 15):
            total = total + z_recv[c, m]
        where = pl.ds(pl.multiple_of(c * width, 128), width)
        total_ref[:, where] = total
        total = prev_ref[:, where] + total
        squares[...] += total * total

    moves[2].wait()
    moves[3].wait()
    begin(0, first=True)
    for c in range(CHUNKS):
        if c not in (0, EVERY - 1, 1):
            stale_copy(c).start()
    moves[4].start()

    @pl.loop(1, CHUNKS + 8)
    def _(s):
        def stage(lag, run, x_first):
            c = s - lag
            fits = (c % EVERY == EVERY - 1) if x_first else (c % EVERY != EVERY - 1)

            @pl.when((c >= 0) & (c < CHUNKS) & fits)
            def _():
                run(c)

        stage(0, begin, False)
        stage(0, sum_pair, True)

        @pl.when((s + LEAD < CHUNKS) & ((s + LEAD) % EVERY == EVERY - 1))
        def _():
            begin_pair(s + LEAD)

        for i in range(2):

            @pl.when(s == i + 1)
            def _(i=i):
                pl.semaphore_wait(word_sem.at[i], 2)
                if i < 1:
                    tell_z(i + 1)
                else:
                    moves[4].wait()

        stage(1, pass_on, False)
        stage(1, pass_on_pair, True)
        stage(2, sum_y, False)
        stage(2, sum_y_pair, True)
        stage(3, sum_x, False)
        stage(3, pass_on_z, True)
        stage(4, pass_on_z, False)
        stage(5, pass_on_again, True)
        stage(6, pass_on_again, False)
        stage(7, finish, True)
        stage(8, finish, False)

    lanes = squares[0:8, 0:128]
    for i in range(own // 8):
        for j in range(width // 128):
            if i + j > 0:
                lanes = lanes + squares[i * 8 : (i + 1) * 8, j * 128 : (j + 1) * 128]
    lanes = jnp.sum(lanes, axis=0, keepdims=True)
    n_data[0, 0:1, :] = lanes
    n_data[0, 1:2, :] = trigger_ref[...].astype(jnp.float32)

    def n_copy(k):
        return pltpu.make_async_remote_copy(
            n_data.at[0], n_recv_z.at[k - 1], n_send_sem.at[0], n_recv_sem.at[0],
            device_id=at(y, x, z_off(k)), device_id_type=MESH,
        )

    def p_copy(i):
        return pltpu.make_async_remote_copy(
            n_data.at[1], n_recv_p.at[i], n_send_sem.at[1], n_recv_sem.at[1],
            device_id=plane_peer(*plane[i]), device_id_type=MESH,
        )

    for k in (8, 7, 9, 6, 10, 5, 11, 4, 12, 3, 13, 2, 14, 1, 15):
        n_copy(k).start()
    moves[5].start()
    arrived(y_recv.at[pl.ds(0, CHUNKS - X_FIRST // 2)], y_send_sem.at[0])
    arrived(x_recv.at[pl.ds(0, CHUNKS - X_FIRST)], x_send_sem.at[0])
    arrived(pair_recv, x_send_sem.at[1])
    arrived(z_recv, z_send_sem.at[0])
    arrived(n_recv_z, n_recv_sem.at[0])
    n_data[1] = n_data[0] + jnp.sum(n_recv_z[...], axis=0)
    for i in far_first:
        p_copy(i).start()
    arrived(n_recv_z, n_send_sem.at[0])
    moves[5].wait()
    arrived(n_recv_p, n_recv_sem.at[1])
    both = n_data[1] + jnp.sum(n_recv_p[...], axis=0)
    square_total = jnp.sum(both[0:1, :], axis=1, keepdims=True)
    limit = clip_ratio * jnp.sqrt(jnp.full((1, 1), 4 * rows * cols, jnp.float32))
    factor_ref[...] = jnp.minimum(1.0, limit / jnp.sqrt(square_total + epsilon))
    count_ref[...] = jnp.sum(both[1:2, :], axis=1, keepdims=True)

    arrived(n_recv_p, n_send_sem.at[1])


def local(hidden_acts, out_grad, token_ids, trigger, stale, aggregate_prev):
    tokens, rows = hidden_acts.shape[1:]
    cols = out_grad.shape[2]
    width = cols // CHUNKS
    half = rows // (NY * NX)
    own = aggregate_prev.shape[1]
    vmem = pl.BlockSpec(memory_space=pltpu.VMEM)
    hbm = pl.BlockSpec(memory_space=pltpu.HBM)
    bf16, f32 = jnp.bfloat16, jnp.float32
    dma = pltpu.SemaphoreType.DMA
    total, factor, count = pl.pallas_call(
        functools.partial(reduce_kernel, rows, cols),
        out_shape=(
            jax.ShapeDtypeStruct((own, cols), f32),
            jax.ShapeDtypeStruct((1, 1), f32),
            jax.ShapeDtypeStruct((1, 1), f32),
        ),
        in_specs=[hbm] * 6,
        out_specs=(hbm, vmem, vmem),
        scratch_shapes=[
            pltpu.VMEM(token_ids.shape, jnp.int32),
            pltpu.VMEM(trigger.shape, jnp.int32),
            pltpu.VMEM((tokens, cols), bf16),
            pltpu.VMEM((tokens, rows), bf16),
            pltpu.VMEM((own, cols), f32),
            pltpu.VMEM((own, cols), f32),
            pltpu.VMEM((rows, tokens), bf16),
            pltpu.VMEM((tokens, width), bf16),
            pltpu.VMEM((tokens, width), f32),
            pltpu.VMEM((rows // BLOCK, width), f32),
            pltpu.VMEM((CHUNKS, rows, width), bf16),
            pltpu.VMEM((CHUNKS, 6, half, width), bf16),
            pltpu.VMEM((CHUNKS, NX, half, width), f32),
            pltpu.VMEM((CHUNKS, half, width), f32),
            pltpu.VMEM((X_FIRST, NY, half, width), bf16),
            pltpu.VMEM((CHUNKS, NZ, own, width), f32),
            pltpu.VMEM((CHUNKS, 4, own, width), f32),
            pltpu.VMEM((CHUNKS, 15, own, width), f32),
            pltpu.VMEM((own, width), f32),
            pltpu.VMEM((2, 2, 128), f32),
            pltpu.VMEM((NZ - 1, 2, 128), f32),
            pltpu.VMEM((NY * NG * 2 - 1, 2, 128), f32),
            dma((6,)),
            dma((CHUNKS,)),
            dma((1,)),
            dma((CHUNKS, 3)),
            dma((2,)),
            dma((CHUNKS,)),
            dma((X_FIRST,)),
            dma((1,)),
            dma((CHUNKS, 3)),
            dma((2,)),
            dma((2,)),
            pltpu.SemaphoreType.REGULAR((2,)),
        ],
        compiler_params=pltpu.CompilerParams(
            collective_id=0, has_side_effects=True, vmem_limit_bytes=66_900_000
        ),
        name="reduce_deltas",
    )(token_ids, trigger, out_grad[0], hidden_acts[0], aggregate_prev[0], stale[0])
    aggregate = aggregate_prev[0] + total
    return (aggregate[None], (aggregate * factor)[None], count[0, 0])


def solution(mesh):
    in_specs = (
        P("dp", None, "shard"),
        P("dp", None, None),
        P("dp", None),
        P("dp", "shard"),
        P("dp", "shard", None),
        P("shard", "dp", None),
    )
    out_specs = (P("shard", "dp", None), P("shard", "dp", None), P())
    return jax.shard_map(local, mesh=mesh, in_specs=in_specs, out_specs=out_specs, check_vma=False)
```

```python
import functools

import jax
import jax.numpy as jnp
from jax import lax
from jax.experimental import pallas as pl
from jax.experimental.pallas import tpu as pltpu
from jax.sharding import PartitionSpec as P

BLOCK = 16
NY, NX, NZ = 4, 2, 16
NG = 2 * NX
CHUNKS = 8
EVERY = 4
X_FIRST = CHUNKS // EVERY
LEAD = 2
MESH = pl.DeviceIdType.MESH

clip_ratio = 0.25
epsilon = 1e-06


def reduce_kernel(
    rows, cols,
    ids_hbm, trigger_hbm, grad_hbm, hidden_hbm, prev_hbm, stale_hbm,
    total_hbm, factor_ref, count_ref,
    ids_ref, trigger_ref, grad_ref, hidden_ref, prev_ref,
    total_ref, hidden_t, masked, keep, flags, delta, y_recv, x_data, x_recv, pair_recv, z_data, z_mid, z_recv, squares,
    n_data, n_recv_z, n_recv_p,
    input_sem, stale_sem, y_send_sem, y_recv_sem, x_send_sem, x_recv_sem, pair_sem, z_send_sem, z_recv_sem,
    n_send_sem, n_recv_sem, word_sem,
):
    tokens = hidden_ref.shape[0]
    width = cols // CHUNKS
    half = rows // (NY * NX)
    own = half // NZ
    me = lax.axis_index("dp")
    shard = lax.axis_index("shard")
    y = me // (NX * NZ)
    x = (me // NZ) % NX
    z = me % NZ
    core = shard % 2
    group_x = (shard // 2) * NX + x
    y_right, y_left, y_far = (y + 1) % NY, (y + NY - 1) % NY, (y + 2) % NY

    def at(yy, xx, zz):
        return {"dp": yy * (NX * NZ) + xx * NZ + zz}

    right, left = at(y_right, x, z), at(y_left, x, z)
    across = at(y, 1 - x, z)

    def z_off(k):
        return (z + NZ + k) % NZ

    plane = [(oy, ox, oc) for oy in range(NY) for ox in range(NG) for oc in range(2)][1:]

    far_first = sorted(
        range(len(plane)), key=lambda i: -(min(plane[i][0], NY - plane[i][0]) + min(plane[i][1], NG - plane[i][1]))
    )

    def plane_peer(oy, ox, oc):
        yy, xx, cc = (y + oy) % NY, (group_x + ox) % NG, (core + oc) % 2
        return {"dp": yy * (NX * NZ) + (xx % NX) * NZ + z, "shard": (xx // NX) * 2 + cc}

    moves = [
        pltpu.make_async_copy(source, target, input_sem.at[i])
        for i, (source, target) in enumerate((
            (ids_hbm, ids_ref), (trigger_hbm, trigger_ref), (grad_hbm, grad_ref),
            (hidden_hbm, hidden_ref), (prev_hbm, prev_ref), (total_ref, total_hbm),
        ))
    ]

    def stale_copy(c):
        return pltpu.make_async_copy(
            stale_hbm.at[:, pl.ds(pl.multiple_of(c * width, 128), width)],
            delta.at[c], stale_sem.at[c],
        )

    for copy in moves[:4]:
        copy.start()
    for c in (0, EVERY - 1, 1):
        stale_copy(c).start()

    barrier = pltpu.get_barrier_semaphore()
    near = [right, left, across, at(y, x, z_off(1)), at(y, x, z_off(-1))]
    near += [plane_peer(0, 0, 1), plane_peer(0, NX, 0), plane_peer(0, NX, 1)]
    for peer in near:
        pl.semaphore_signal(barrier, inc=1, device_id=peer, device_id_type=MESH)

    def tell_z(i):
        for k in (1, -1):
            pl.semaphore_signal(word_sem.at[i], inc=1, device_id=at(y, x, z_off(k)), device_id_type=MESH)

    moves[0].wait()
    moves[1].wait()
    real = jnp.broadcast_to(ids_ref[...], (tokens, tokens)).T != 0
    real = jnp.where(real, 1.0, 0.0)
    blocks = rows // BLOCK
    sent = jnp.broadcast_to(trigger_ref[...].astype(jnp.float32), (blocks, blocks)).T
    for j in range(width // 128):
        keep[:, j * 128 : (j + 1) * 128] = real
        flags[:, j * 128 : (j + 1) * 128] = sent
    squares[...] = jnp.zeros_like(squares)

    def first_row(yy, xx):
        return pl.multiple_of(yy * (NX * half) + xx * half, half)

    def rows_of(yy, xx):
        return pl.ds(first_row(yy, xx), half)

    def y_copy(c, m):
        yy, xx, device = (
            (y_far, 0, left), (y_far, 1, right),
            (y_left, 1, left), (y_right, 0, right),
            (y_left, 0, left), (y_right, 1, right),
        )[m]
        return pltpu.make_async_remote_copy(
            delta.at[c, rows_of(yy, xx)], y_recv.at[c, m], y_send_sem.at[0], y_recv_sem.at[c, min(m, 2)],
            device_id=device, device_id_type=MESH,
        )

    def x_copy(c):
        return pltpu.make_async_remote_copy(
            x_data.at[c, 1 - x], x_recv.at[c], x_send_sem.at[0], x_recv_sem.at[c],
            device_id=across, device_id_type=MESH,
        )

    z_messages = (
        (-8, -2, 0, None), (-7, -1, 0, None), (7, 1, 0, None),
        (-5, -2, 1, None), (-4, -1, 1, None), (None, -3, 1, 0),
        (5, 2, 1, None), (4, 1, 1, None), (None, 3, 1, 1),
        (-2, -2, 2, None), (-1, -1, 2, None), (None, -3, 2, 2),
        (2, 2, 2, None), (1, 1, 2, None), (None, 3, 2, 3),
    )

    def z_copy(c, m):
        k, hops, batch, middle = z_messages[m]
        source = z_data.at[c, z_off(k)] if middle is None else z_mid.at[c, middle]
        return pltpu.make_async_remote_copy(
            source, z_recv.at[c, m], z_send_sem.at[0], z_recv_sem.at[c, batch],
            device_id=at(y, x, z_off(hops)), device_id_type=MESH,
        )

    def arrived(ref, sem):
        pltpu.make_async_copy(ref, ref, sem).wait()

    def compute(c, yy, xx, first):
        start = first_row(yy, xx)
        if first:
            for j in range(half // 128):
                part = pl.ds(pl.multiple_of(start + j * 128, 128), 128)
                hidden_t[part, :] = hidden_ref[:, part].T
        gradient = jnp.dot(
            hidden_t[pl.ds(start, half), :], masked[...], preferred_element_type=jnp.float32
        )
        diff = gradient - delta[c, pl.ds(start, half), :].astype(jnp.float32)
        for i in range(half // BLOCK):
            flag = flags[pl.ds(start // BLOCK + i, 1), :]
            delta[c, pl.ds(start + i * BLOCK, BLOCK), :] = (
                flag * diff[i * BLOCK : (i + 1) * BLOCK]
            ).astype(jnp.bfloat16)

    def prepare(c):
        part = grad_ref[:, pl.ds(pl.multiple_of(c * width, 128), width)]
        masked[...] = (part.astype(jnp.float32) * keep[...]).astype(jnp.bfloat16)
        stale_copy(c).wait()

    def begin(c, first=False):
        prepare(c)
        compute(c, y_far, 0, first)
        compute(c, y_far, 1, first)
        if first:
            pl.semaphore_wait(barrier, len(near))
            tell_z(0)
        y_copy(c, 0).start()
        compute(c, y_left, 1, first)
        y_copy(c, 1).start()
        compute(c, y_right, 0, first)
        y_copy(c, 2).start()
        compute(c, y_left, 0, first)
        y_copy(c, 3).start()
        compute(c, y_right, 1, first)
        compute(c, y, 0, first)
        compute(c, y, 1, first)

    def pass_on(c):
        for m, yy, xx in ((0, y_left, 0), (1, y_right, 1)):
            y_copy(c, m).wait_recv()
            where = rows_of(yy, xx)
            total = delta[c, where, :].astype(jnp.float32) + y_recv[c, m].astype(jnp.float32)
            delta[c, where, :] = total.astype(jnp.bfloat16)
            y_copy(c, m + 4).start()

    def sum_y(c):
        arrived(y_recv.at[c, pl.ds(2, 4)], y_recv_sem.at[c, 2])
        for xx, first, second in ((0, 3, 4), (1, 2, 5)):
            x_data[c, xx] = (
                delta[c, rows_of(y, xx), :].astype(jnp.float32)
                + y_recv[c, first].astype(jnp.float32)
                + y_recv[c, second].astype(jnp.float32)
            )
        x_copy(c).start()

    def pair_copy(c, yy):
        return pltpu.make_async_remote_copy(
            delta.at[c, rows_of(yy, 1 - x)], pair_recv.at[c // EVERY, yy],
            x_send_sem.at[1], pair_sem.at[c // EVERY],
            device_id=across, device_id_type=MESH,
        )

    quarter = half // 2

    def part_of(yy, h):
        return pl.ds(pl.multiple_of(first_row(yy, x) + h * quarter, quarter), quarter)

    def y_pair_copy(c, m):
        yy, h, device = (
            (y_far, 0, left), (y_far, 1, right),
            (y_left, 1, left), (y_right, 0, right),
            (y_left, 0, left), (y_right, 1, right),
        )[m]
        return pltpu.make_async_remote_copy(
            delta.at[c, part_of(yy, h)], y_recv.at[c, m, pl.ds(0, quarter)],
            y_send_sem.at[0], y_recv_sem.at[c, min(m, 2)],
            device_id=device, device_id_type=MESH,
        )

    def begin_pair(c):
        prepare(c)
        for yy in range(NY):
            compute(c, yy, 1 - x, False)
            if yy > 0:
                pair_copy(c, yy - 1).start()
        compute(c, 0, x, False)
        pair_copy(c, NY - 1).start()
        for yy in range(1, NY):
            compute(c, yy, x, False)

    def sum_pair(c):
        arrived(pair_recv.at[c // EVERY], pair_sem.at[c // EVERY])

        def both(yy):
            return delta[c, rows_of(yy, x), :].astype(jnp.float32) + pair_recv[c // EVERY, yy].astype(jnp.float32)

        for yy in (y_far, y_left, y_right):
            delta[c, rows_of(yy, x), :] = both(yy).astype(jnp.bfloat16)
        for m in range(4):
            y_pair_copy(c, m).start()
        x_data[c, 0] = both(y)

    def pass_on_pair(c):
        for m, yy, h in ((0, y_left, 0), (1, y_right, 1)):
            y_pair_copy(c, m).wait_recv()
            where = part_of(yy, h)
            total = delta[c, where, :].astype(jnp.float32) + y_recv[c, m, pl.ds(0, quarter), :].astype(jnp.float32)
            delta[c, where, :] = total.astype(jnp.bfloat16)
            y_pair_copy(c, m + 4).start()

    def send_z(c):
        for m in (0, 2, 1, 3, 6, 4, 7, 9, 12, 10, 13):
            z_copy(c, m).start()

    def sum_y_pair(c):
        arrived(y_recv.at[c, pl.ds(2, 2)], y_recv_sem.at[c, 2])
        for h, first, second in ((0, 3, 4), (1, 2, 5)):
            for k in range(NZ // 2):
                part = pl.ds(k * own, own)
                z_data[c, h * (NZ // 2) + k] = (
                    x_data[c, 0, pl.ds(h * quarter + k * own, own), :]
                    + y_recv[c, first, part, :].astype(jnp.float32)
                    + y_recv[c, second, part, :].astype(jnp.float32)
                )
        send_z(c)

    def sum_x(c):
        x_copy(c).wait_recv()
        for k in range(NZ):
            part = pl.ds(k * own, own)
            z_data[c, k] = x_data[c, x, part, :] + x_recv[c, part, :]
        send_z(c)

    def pass_on_z(c):
        arrived(z_recv.at[c, pl.ds(0, 3)], z_recv_sem.at[c, 0])
        z_mid[c, 0] = z_data[c, z_off(-6)] + z_recv[c, 0] + z_recv[c, 1]
        z_copy(c, 5).start()
        z_mid[c, 1] = z_data[c, z_off(6)] + z_recv[c, 2]
        z_copy(c, 8).start()

    def pass_on_again(c):
        arrived(z_recv.at[c, pl.ds(3, 6)], z_recv_sem.at[c, 1])
        z_mid[c, 2] = z_data[c, z_off(-3)] + z_recv[c, 3] + z_recv[c, 4] + z_recv[c, 5]
        z_copy(c, 11).start()
        z_mid[c, 3] = z_data[c, z_off(3)] + z_recv[c, 6] + z_recv[c, 7] + z_recv[c, 8]
        z_copy(c, 14).start()

    def finish(c):
        arrived(z_recv.at[c, pl.ds(9, 6)], z_recv_sem.at[c, 2])
        total = z_data[c, z]
        for m in range(9, 15):
            total = total + z_recv[c, m]
        where = pl.ds(pl.multiple_of(c * width, 128), width)
        total_ref[:, where] = total
        total = prev_ref[:, where] + total
        squares[...] += total * total

    moves[2].wait()
    moves[3].wait()
    begin(0, first=True)
    for c in range(CHUNKS):
        if c not in (0, EVERY - 1, 1):
            stale_copy(c).start()
    moves[4].start()

    @pl.loop(1, CHUNKS + 8)
    def _(s):
        def stage(lag, run, x_first):
            c = s - lag
            fits = (c % EVERY == EVERY - 1) if x_first else (c % EVERY != EVERY - 1)

            @pl.when((c >= 0) & (c < CHUNKS) & fits)
            def _():
                run(c)

        stage(0, begin, False)
        stage(0, sum_pair, True)

        @pl.when((s + LEAD < CHUNKS) & ((s + LEAD) % EVERY == EVERY - 1))
        def _():
            begin_pair(s + LEAD)

        for i in range(2):

            @pl.when(s == i + 1)
            def _(i=i):
                pl.semaphore_wait(word_sem.at[i], 2)
                if i < 1:
                    tell_z(i + 1)
                else:
                    moves[4].wait()

        stage(1, pass_on, False)
        stage(1, pass_on_pair, True)
        stage(2, sum_y, False)
        stage(2, sum_y_pair, True)
        stage(3, sum_x, False)
        stage(3, pass_on_z, True)
        stage(4, pass_on_z, False)
        stage(5, pass_on_again, True)
        stage(6, pass_on_again, False)
        stage(7, finish, True)
        stage(8, finish, False)

    lanes = squares[0:8, 0:128]
    for i in range(own // 8):
        for j in range(width // 128):
            if i + j > 0:
                lanes = lanes + squares[i * 8 : (i + 1) * 8, j * 128 : (j + 1) * 128]
    lanes = jnp.sum(lanes, axis=0, keepdims=True)
    n_data[0, 0:1, :] = lanes
    n_data[0, 1:2, :] = trigger_ref[...].astype(jnp.float32)

    def n_copy(k):
        return pltpu.make_async_remote_copy(
            n_data.at[0], n_recv_z.at[k - 1], n_send_sem.at[0], n_recv_sem.at[0],
            device_id=at(y, x, z_off(k)), device_id_type=MESH,
        )

    def p_copy(i):
        return pltpu.make_async_remote_copy(
            n_data.at[1], n_recv_p.at[i], n_send_sem.at[1], n_recv_sem.at[1],
            device_id=plane_peer(*plane[i]), device_id_type=MESH,
        )

    for k in (8, 7, 9, 6, 10, 5, 11, 4, 12, 3, 13, 2, 14, 1, 15):
        n_copy(k).start()
    moves[5].start()
    arrived(y_recv.at[pl.ds(0, CHUNKS - X_FIRST // 2)], y_send_sem.at[0])
    arrived(x_recv.at[pl.ds(0, CHUNKS - X_FIRST)], x_send_sem.at[0])
    arrived(pair_recv, x_send_sem.at[1])
    arrived(z_recv, z_send_sem.at[0])
    arrived(n_recv_z, n_recv_sem.at[0])
    n_data[1] = n_data[0] + jnp.sum(n_recv_z[...], axis=0)
    for i in far_first:
        p_copy(i).start()
    arrived(n_recv_z, n_send_sem.at[0])
    moves[5].wait()
    arrived(n_recv_p, n_recv_sem.at[1])
    both = n_data[1] + jnp.sum(n_recv_p[...], axis=0)
    square_total = jnp.sum(both[0:1, :], axis=1, keepdims=True)
    limit = clip_ratio * jnp.sqrt(jnp.full((1, 1), 4 * rows * cols, jnp.float32))
    factor_ref[...] = jnp.minimum(1.0, limit / jnp.sqrt(square_total + epsilon))
    count_ref[...] = jnp.sum(both[1:2, :], axis=1, keepdims=True)

    arrived(n_recv_p, n_send_sem.at[1])


def output_kernel(
    total_hbm, prev_hbm, factor_hbm, count_hbm, aggregate_hbm, update_hbm, triggered_hbm,
    total, prev, factor, count, update, sems,
):
    loads = [
        pltpu.make_async_copy(source, target, sems.at[i])
        for i, (source, target) in enumerate(
            ((total_hbm, total), (prev_hbm, prev), (factor_hbm, factor), (count_hbm, count))
        )
    ]
    stores = [
        pltpu.make_async_copy(source, target, sems.at[4 + i])
        for i, (source, target) in enumerate(
            ((total, aggregate_hbm), (update, update_hbm), (count, triggered_hbm))
        )
    ]
    for copy in loads:
        copy.start()
    for copy in loads:
        copy.wait()
    stores[2].start()
    aggregate = prev[...] + total[...]
    update[...] = aggregate * factor[...]
    total[...] = aggregate
    stores[1].start()
    stores[0].start()
    for copy in stores:
        copy.wait()


def local(hidden_acts, out_grad, token_ids, trigger, stale, aggregate_prev):
    tokens, rows = hidden_acts.shape[1:]
    cols = out_grad.shape[2]
    width = cols // CHUNKS
    half = rows // (NY * NX)
    own = aggregate_prev.shape[1]
    vmem = pl.BlockSpec(memory_space=pltpu.VMEM)
    hbm = pl.BlockSpec(memory_space=pltpu.HBM)
    bf16, f32 = jnp.bfloat16, jnp.float32
    dma = pltpu.SemaphoreType.DMA
    total, factor, count = pl.pallas_call(
        functools.partial(reduce_kernel, rows, cols),
        out_shape=(
            jax.ShapeDtypeStruct((own, cols), f32),
            jax.ShapeDtypeStruct((1, 1), f32),
            jax.ShapeDtypeStruct((1, 1), f32),
        ),
        in_specs=[hbm] * 6,
        out_specs=(hbm, vmem, vmem),
        scratch_shapes=[
            pltpu.VMEM(token_ids.shape, jnp.int32),
            pltpu.VMEM(trigger.shape, jnp.int32),
            pltpu.VMEM((tokens, cols), bf16),
            pltpu.VMEM((tokens, rows), bf16),
            pltpu.VMEM((own, cols), f32),
            pltpu.VMEM((own, cols), f32),
            pltpu.VMEM((rows, tokens), bf16),
            pltpu.VMEM((tokens, width), bf16),
            pltpu.VMEM((tokens, width), f32),
            pltpu.VMEM((rows // BLOCK, width), f32),
            pltpu.VMEM((CHUNKS, rows, width), bf16),
            pltpu.VMEM((CHUNKS, 6, half, width), bf16),
            pltpu.VMEM((CHUNKS, NX, half, width), f32),
            pltpu.VMEM((CHUNKS, half, width), f32),
            pltpu.VMEM((X_FIRST, NY, half, width), bf16),
            pltpu.VMEM((CHUNKS, NZ, own, width), f32),
            pltpu.VMEM((CHUNKS, 4, own, width), f32),
            pltpu.VMEM((CHUNKS, 15, own, width), f32),
            pltpu.VMEM((own, width), f32),
            pltpu.VMEM((2, 2, 128), f32),
            pltpu.VMEM((NZ - 1, 2, 128), f32),
            pltpu.VMEM((NY * NG * 2 - 1, 2, 128), f32),
            dma((6,)),
            dma((CHUNKS,)),
            dma((1,)),
            dma((CHUNKS, 3)),
            dma((2,)),
            dma((CHUNKS,)),
            dma((X_FIRST,)),
            dma((1,)),
            dma((CHUNKS, 3)),
            dma((2,)),
            dma((2,)),
            pltpu.SemaphoreType.REGULAR((2,)),
        ],
        compiler_params=pltpu.CompilerParams(
            collective_id=0, has_side_effects=True, vmem_limit_bytes=66_900_000
        ),
        name="reduce_deltas",
    )(token_ids, trigger, out_grad[0], hidden_acts[0], aggregate_prev[0], stale[0])
    aggregate, update, triggered = pl.pallas_call(
        output_kernel,
        out_shape=(
            jax.ShapeDtypeStruct((own, cols), f32),
            jax.ShapeDtypeStruct((own, cols), f32),
            jax.ShapeDtypeStruct((1, 1), f32),
        ),
        in_specs=[hbm] * 4,
        out_specs=(hbm,) * 3,
        scratch_shapes=[
            pltpu.VMEM((own, cols), f32),
            pltpu.VMEM((own, cols), f32),
            pltpu.VMEM((1, 1), f32),
            pltpu.VMEM((1, 1), f32),
            pltpu.VMEM((own, cols), f32),
            dma((7,)),
        ],
        compiler_params=pltpu.CompilerParams(vmem_limit_bytes=67_000_000),
        name="clip",
    )(total, aggregate_prev[0], factor, count)
    return (aggregate[None], update[None], triggered[0, 0])


def solution(mesh):
    in_specs = (
        P("dp", None, "shard"),
        P("dp", None, None),
        P("dp", None),
        P("dp", "shard"),
        P("dp", "shard", None),
        P("shard", "dp", None),
    )
    out_specs = (P("shard", "dp", None), P("shard", "dp", None), P())
    return jax.shard_map(local, mesh=mesh, in_specs=in_specs, out_specs=out_specs, check_vma=False)
```

```python
import functools

import jax
import jax.numpy as jnp
from jax import lax
from jax.experimental import pallas as pl
from jax.experimental.pallas import tpu as pltpu
from jax.sharding import PartitionSpec as P

BLOCK = 16
NY, NX, NZ = 4, 2, 16
NG = 2 * NX
CHUNKS = 8
EVERY = 4
X_FIRST = CHUNKS // EVERY
LEAD = 2
MESH = pl.DeviceIdType.MESH

clip_ratio = 0.25
epsilon = 1e-06


def reduce_kernel(
    rows, cols,
    ids_hbm, trigger_hbm, grad_hbm, hidden_hbm, prev_hbm, stale_hbm,
    total_hbm, factor_ref, count_ref,
    ids_ref, trigger_ref, grad_ref, hidden_ref, prev_ref,
    total_ref, hidden_t, masked, keep, flags, delta, y_recv, x_data, x_recv, pair_recv, z_data, z_mid, z_recv, squares,
    n_data, n_recv_z, n_recv_p,
    input_sem, stale_sem, y_send_sem, y_recv_sem, x_send_sem, x_recv_sem, pair_sem, z_send_sem, z_recv_sem,
    n_send_sem, n_recv_sem, word_sem,
):
    tokens = hidden_ref.shape[0]
    width = cols // CHUNKS
    half = rows // (NY * NX)
    own = half // NZ
    me = lax.axis_index("dp")
    shard = lax.axis_index("shard")
    y = me // (NX * NZ)
    x = (me // NZ) % NX
    z = me % NZ
    core = shard % 2
    group_x = (shard // 2) * NX + x
    y_right, y_left, y_far = (y + 1) % NY, (y + NY - 1) % NY, (y + 2) % NY

    def at(yy, xx, zz):
        return {"dp": yy * (NX * NZ) + xx * NZ + zz}

    right, left = at(y_right, x, z), at(y_left, x, z)
    across = at(y, 1 - x, z)

    def z_off(k):
        return (z + NZ + k) % NZ

    plane = [(oy, ox, oc) for oy in range(NY) for ox in range(NG) for oc in range(2)][1:]

    far_first = sorted(
        range(len(plane)), key=lambda i: -(min(plane[i][0], NY - plane[i][0]) + min(plane[i][1], NG - plane[i][1]))
    )

    def plane_peer(oy, ox, oc):
        yy, xx, cc = (y + oy) % NY, (group_x + ox) % NG, (core + oc) % 2
        return {"dp": yy * (NX * NZ) + (xx % NX) * NZ + z, "shard": (xx // NX) * 2 + cc}

    moves = [
        pltpu.make_async_copy(source, target, input_sem.at[i])
        for i, (source, target) in enumerate((
            (ids_hbm, ids_ref), (trigger_hbm, trigger_ref), (grad_hbm, grad_ref),
            (hidden_hbm, hidden_ref), (prev_hbm, prev_ref), (total_ref, total_hbm),
        ))
    ]

    def stale_copy(c):
        return pltpu.make_async_copy(
            stale_hbm.at[:, pl.ds(pl.multiple_of(c * width, 128), width)],
            delta.at[c], stale_sem.at[c],
        )

    for copy in moves[:4]:
        copy.start()
    stale_copy(0).start()

    barrier = pltpu.get_barrier_semaphore()
    near = [right, left, across, at(y, x, z_off(1)), at(y, x, z_off(-1))]
    near += [plane_peer(0, 0, 1), plane_peer(0, NX, 0), plane_peer(0, NX, 1)]
    for peer in near:
        pl.semaphore_signal(barrier, inc=1, device_id=peer, device_id_type=MESH)

    def tell_z(i):
        for k in (1, -1):
            pl.semaphore_signal(word_sem.at[i], inc=1, device_id=at(y, x, z_off(k)), device_id_type=MESH)

    moves[0].wait()
    moves[1].wait()
    real = jnp.broadcast_to(ids_ref[...], (tokens, tokens)).T != 0
    real = jnp.where(real, 1.0, 0.0)
    blocks = rows // BLOCK
    sent = jnp.broadcast_to(trigger_ref[...].astype(jnp.float32), (blocks, blocks)).T
    for j in range(width // 128):
        keep[:, j * 128 : (j + 1) * 128] = real
        flags[:, j * 128 : (j + 1) * 128] = sent
    squares[...] = jnp.zeros_like(squares)

    def first_row(yy, xx):
        return pl.multiple_of(yy * (NX * half) + xx * half, half)

    def rows_of(yy, xx):
        return pl.ds(first_row(yy, xx), half)

    def y_copy(c, m):
        yy, xx, device = (
            (y_far, 0, left), (y_far, 1, right),
            (y_left, 1, left), (y_right, 0, right),
            (y_left, 0, left), (y_right, 1, right),
        )[m]
        return pltpu.make_async_remote_copy(
            delta.at[c, rows_of(yy, xx)], y_recv.at[c, m], y_send_sem.at[0], y_recv_sem.at[c, min(m, 2)],
            device_id=device, device_id_type=MESH,
        )

    def x_copy(c):
        return pltpu.make_async_remote_copy(
            x_data.at[c, 1 - x], x_recv.at[c], x_send_sem.at[0], x_recv_sem.at[c],
            device_id=across, device_id_type=MESH,
        )

    z_messages = (
        (-8, -2, 0, None), (-7, -1, 0, None), (7, 1, 0, None),
        (-5, -2, 1, None), (-4, -1, 1, None), (None, -3, 1, 0),
        (5, 2, 1, None), (4, 1, 1, None), (None, 3, 1, 1),
        (-2, -2, 2, None), (-1, -1, 2, None), (None, -3, 2, 2),
        (2, 2, 2, None), (1, 1, 2, None), (None, 3, 2, 3),
    )

    def z_copy(c, m):
        k, hops, batch, middle = z_messages[m]
        source = z_data.at[c, z_off(k)] if middle is None else z_mid.at[c, middle]
        return pltpu.make_async_remote_copy(
            source, z_recv.at[c, m], z_send_sem.at[0], z_recv_sem.at[c, batch],
            device_id=at(y, x, z_off(hops)), device_id_type=MESH,
        )

    def arrived(ref, sem):
        pltpu.make_async_copy(ref, ref, sem).wait()

    def compute(c, yy, xx, first):
        start = first_row(yy, xx)
        if first:
            for j in range(half // 128):
                part = pl.ds(pl.multiple_of(start + j * 128, 128), 128)
                hidden_t[part, :] = hidden_ref[:, part].T
        gradient = jnp.dot(
            hidden_t[pl.ds(start, half), :], masked[...], preferred_element_type=jnp.float32
        )
        diff = gradient - delta[c, pl.ds(start, half), :].astype(jnp.float32)
        for i in range(half // BLOCK):
            flag = flags[pl.ds(start // BLOCK + i, 1), :]
            delta[c, pl.ds(start + i * BLOCK, BLOCK), :] = (
                flag * diff[i * BLOCK : (i + 1) * BLOCK]
            ).astype(jnp.bfloat16)

    def prepare(c):
        part = grad_ref[:, pl.ds(pl.multiple_of(c * width, 128), width)]
        masked[...] = (part.astype(jnp.float32) * keep[...]).astype(jnp.bfloat16)
        stale_copy(c).wait()

    def begin(c, first=False):
        prepare(c)
        if first:
            for later in sorted(range(1, CHUNKS), key=lambda k: (k > 1, k != EVERY - 1)):
                stale_copy(later).start()
        compute(c, y_far, 0, first)
        compute(c, y_far, 1, first)
        if first:
            pl.semaphore_wait(barrier, len(near))
            tell_z(0)
        y_copy(c, 0).start()
        compute(c, y_left, 1, first)
        y_copy(c, 1).start()
        compute(c, y_right, 0, first)
        y_copy(c, 2).start()
        compute(c, y_left, 0, first)
        y_copy(c, 3).start()
        compute(c, y_right, 1, first)
        compute(c, y, 0, first)
        compute(c, y, 1, first)

    def pass_on(c):
        for m, yy, xx in ((0, y_left, 0), (1, y_right, 1)):
            y_copy(c, m).wait_recv()
            where = rows_of(yy, xx)
            total = delta[c, where, :].astype(jnp.float32) + y_recv[c, m].astype(jnp.float32)
            delta[c, where, :] = total.astype(jnp.bfloat16)
            y_copy(c, m + 4).start()

    def sum_y(c):
        arrived(y_recv.at[c, pl.ds(2, 4)], y_recv_sem.at[c, 2])
        for xx, first, second in ((0, 3, 4), (1, 2, 5)):
            x_data[c, xx] = (
                delta[c, rows_of(y, xx), :].astype(jnp.float32)
                + y_recv[c, first].astype(jnp.float32)
                + y_recv[c, second].astype(jnp.float32)
            )
        x_copy(c).start()

    def pair_copy(c, yy):
        return pltpu.make_async_remote_copy(
            delta.at[c, rows_of(yy, 1 - x)], pair_recv.at[c // EVERY, yy],
            x_send_sem.at[1], pair_sem.at[c // EVERY],
            device_id=across, device_id_type=MESH,
        )

    quarter = half // 2

    def part_of(yy, h):
        return pl.ds(pl.multiple_of(first_row(yy, x) + h * quarter, quarter), quarter)

    def y_pair_copy(c, m):
        yy, h, device = (
            (y_far, 0, left), (y_far, 1, right),
            (y_left, 1, left), (y_right, 0, right),
            (y_left, 0, left), (y_right, 1, right),
        )[m]
        return pltpu.make_async_remote_copy(
            delta.at[c, part_of(yy, h)], y_recv.at[c, m, pl.ds(0, quarter)],
            y_send_sem.at[0], y_recv_sem.at[c, min(m, 2)],
            device_id=device, device_id_type=MESH,
        )

    def begin_pair(c):
        prepare(c)
        for yy in range(NY):
            compute(c, yy, 1 - x, False)
            if yy > 0:
                pair_copy(c, yy - 1).start()
        compute(c, 0, x, False)
        pair_copy(c, NY - 1).start()
        for yy in range(1, NY):
            compute(c, yy, x, False)

    def sum_pair(c):
        arrived(pair_recv.at[c // EVERY], pair_sem.at[c // EVERY])

        def both(yy):
            return delta[c, rows_of(yy, x), :].astype(jnp.float32) + pair_recv[c // EVERY, yy].astype(jnp.float32)

        for yy in (y_far, y_left, y_right):
            delta[c, rows_of(yy, x), :] = both(yy).astype(jnp.bfloat16)
        for m in range(4):
            y_pair_copy(c, m).start()
        x_data[c, 0] = both(y)

    def pass_on_pair(c):
        for m, yy, h in ((0, y_left, 0), (1, y_right, 1)):
            y_pair_copy(c, m).wait_recv()
            where = part_of(yy, h)
            total = delta[c, where, :].astype(jnp.float32) + y_recv[c, m, pl.ds(0, quarter), :].astype(jnp.float32)
            delta[c, where, :] = total.astype(jnp.bfloat16)
            y_pair_copy(c, m + 4).start()

    def send_z(c):
        for m in (0, 2, 1, 3, 6, 4, 7, 9, 12, 10, 13):
            z_copy(c, m).start()

    def sum_y_pair(c):
        arrived(y_recv.at[c, pl.ds(2, 2)], y_recv_sem.at[c, 2])
        for h, first, second in ((0, 3, 4), (1, 2, 5)):
            for k in range(NZ // 2):
                part = pl.ds(k * own, own)
                z_data[c, h * (NZ // 2) + k] = (
                    x_data[c, 0, pl.ds(h * quarter + k * own, own), :]
                    + y_recv[c, first, part, :].astype(jnp.float32)
                    + y_recv[c, second, part, :].astype(jnp.float32)
                )
        send_z(c)

    def sum_x(c):
        x_copy(c).wait_recv()
        for k in range(NZ):
            part = pl.ds(k * own, own)
            z_data[c, k] = x_data[c, x, part, :] + x_recv[c, part, :]
        send_z(c)

    def pass_on_z(c):
        arrived(z_recv.at[c, pl.ds(0, 3)], z_recv_sem.at[c, 0])
        z_mid[c, 0] = z_data[c, z_off(-6)] + z_recv[c, 0] + z_recv[c, 1]
        z_copy(c, 5).start()
        z_mid[c, 1] = z_data[c, z_off(6)] + z_recv[c, 2]
        z_copy(c, 8).start()

    def pass_on_again(c):
        arrived(z_recv.at[c, pl.ds(3, 6)], z_recv_sem.at[c, 1])
        z_mid[c, 2] = z_data[c, z_off(-3)] + z_recv[c, 3] + z_recv[c, 4] + z_recv[c, 5]
        z_copy(c, 11).start()
        z_mid[c, 3] = z_data[c, z_off(3)] + z_recv[c, 6] + z_recv[c, 7] + z_recv[c, 8]
        z_copy(c, 14).start()

    def finish(c):
        arrived(z_recv.at[c, pl.ds(9, 6)], z_recv_sem.at[c, 2])
        total = z_data[c, z]
        for m in range(9, 15):
            total = total + z_recv[c, m]
        where = pl.ds(pl.multiple_of(c * width, 128), width)
        total_ref[:, where] = total
        total = prev_ref[:, where] + total
        squares[...] += total * total

    moves[2].wait()
    moves[3].wait()
    begin(0, first=True)
    moves[4].start()

    @pl.loop(1, CHUNKS + 9)
    def _(s):
        def stage(lag, run, x_first):
            c = s - lag
            fits = (c % EVERY == EVERY - 1) if x_first else (c % EVERY != EVERY - 1)

            @pl.when((c >= 0) & (c < CHUNKS) & fits)
            def _():
                run(c)

        stage(0, begin, False)
        stage(0, sum_pair, True)

        @pl.when((s + LEAD < CHUNKS) & ((s + LEAD) % EVERY == EVERY - 1))
        def _():
            begin_pair(s + LEAD)

        for i in range(2):

            @pl.when(s == i + 1)
            def _(i=i):
                pl.semaphore_wait(word_sem.at[i], 2)
                if i < 1:
                    tell_z(i + 1)
                else:
                    moves[4].wait()

        stage(1, pass_on, False)
        stage(1, pass_on_pair, True)
        stage(2, sum_y, False)
        stage(2, sum_y_pair, True)
        stage(4, sum_x, False)
        stage(3, pass_on_z, True)
        stage(5, pass_on_z, False)
        stage(5, pass_on_again, True)
        stage(7, pass_on_again, False)
        stage(7, finish, True)
        stage(9, finish, False)

    lanes = squares[0:8, 0:128]
    for i in range(own // 8):
        for j in range(width // 128):
            if i + j > 0:
                lanes = lanes + squares[i * 8 : (i + 1) * 8, j * 128 : (j + 1) * 128]
    lanes = jnp.sum(lanes, axis=0, keepdims=True)
    n_data[0, 0:1, :] = lanes
    n_data[0, 1:2, :] = trigger_ref[...].astype(jnp.float32)

    def n_copy(k):
        return pltpu.make_async_remote_copy(
            n_data.at[0], n_recv_z.at[k - 1], n_send_sem.at[0], n_recv_sem.at[0],
            device_id=at(y, x, z_off(k)), device_id_type=MESH,
        )

    def p_copy(i):
        return pltpu.make_async_remote_copy(
            n_data.at[1], n_recv_p.at[i], n_send_sem.at[1], n_recv_sem.at[1],
            device_id=plane_peer(*plane[i]), device_id_type=MESH,
        )

    for k in (8, 7, 9, 6, 10, 5, 11, 4, 12, 3, 13, 2, 14, 1, 15):
        n_copy(k).start()
    moves[5].start()
    arrived(y_recv.at[pl.ds(0, CHUNKS - X_FIRST // 2)], y_send_sem.at[0])
    arrived(x_recv.at[pl.ds(0, CHUNKS - X_FIRST)], x_send_sem.at[0])
    arrived(pair_recv, x_send_sem.at[1])
    arrived(z_recv, z_send_sem.at[0])
    arrived(n_recv_z, n_recv_sem.at[0])
    n_data[1] = n_data[0] + jnp.sum(n_recv_z[...], axis=0)
    for i in far_first:
        p_copy(i).start()
    arrived(n_recv_z, n_send_sem.at[0])
    moves[5].wait()
    arrived(n_recv_p, n_recv_sem.at[1])
    both = n_data[1] + jnp.sum(n_recv_p[...], axis=0)
    square_total = jnp.sum(both[0:1, :], axis=1, keepdims=True)
    limit = clip_ratio * jnp.sqrt(jnp.full((1, 1), 4 * rows * cols, jnp.float32))
    factor_ref[...] = jnp.minimum(1.0, limit / jnp.sqrt(square_total + epsilon))
    count_ref[...] = jnp.sum(both[1:2, :], axis=1, keepdims=True)

    arrived(n_recv_p, n_send_sem.at[1])


def output_kernel(
    total_hbm, prev_hbm, factor_hbm, count_hbm, aggregate_hbm, update_hbm, triggered_hbm,
    total, prev, factor, count, update, sems,
):
    loads = [
        pltpu.make_async_copy(source, target, sems.at[i])
        for i, (source, target) in enumerate(
            ((total_hbm, total), (prev_hbm, prev), (factor_hbm, factor), (count_hbm, count))
        )
    ]
    stores = [
        pltpu.make_async_copy(source, target, sems.at[4 + i])
        for i, (source, target) in enumerate(
            ((total, aggregate_hbm), (update, update_hbm), (count, triggered_hbm))
        )
    ]
    for copy in loads:
        copy.start()
    for copy in loads:
        copy.wait()
    stores[2].start()
    aggregate = prev[...] + total[...]
    update[...] = aggregate * factor[...]
    total[...] = aggregate
    stores[1].start()
    stores[0].start()
    for copy in stores:
        copy.wait()


def local(hidden_acts, out_grad, token_ids, trigger, stale, aggregate_prev):
    tokens, rows = hidden_acts.shape[1:]
    cols = out_grad.shape[2]
    width = cols // CHUNKS
    half = rows // (NY * NX)
    own = aggregate_prev.shape[1]
    vmem = pl.BlockSpec(memory_space=pltpu.VMEM)
    hbm = pl.BlockSpec(memory_space=pltpu.HBM)
    bf16, f32 = jnp.bfloat16, jnp.float32
    dma = pltpu.SemaphoreType.DMA
    total, factor, count = pl.pallas_call(
        functools.partial(reduce_kernel, rows, cols),
        out_shape=(
            jax.ShapeDtypeStruct((own, cols), f32),
            jax.ShapeDtypeStruct((1, 1), f32),
            jax.ShapeDtypeStruct((1, 1), f32),
        ),
        in_specs=[hbm] * 6,
        out_specs=(hbm, vmem, vmem),
        scratch_shapes=[
            pltpu.VMEM(token_ids.shape, jnp.int32),
            pltpu.VMEM(trigger.shape, jnp.int32),
            pltpu.VMEM((tokens, cols), bf16),
            pltpu.VMEM((tokens, rows), bf16),
            pltpu.VMEM((own, cols), f32),
            pltpu.VMEM((own, cols), f32),
            pltpu.VMEM((rows, tokens), bf16),
            pltpu.VMEM((tokens, width), bf16),
            pltpu.VMEM((tokens, width), f32),
            pltpu.VMEM((rows // BLOCK, width), f32),
            pltpu.VMEM((CHUNKS, rows, width), bf16),
            pltpu.VMEM((CHUNKS, 6, half, width), bf16),
            pltpu.VMEM((CHUNKS, NX, half, width), f32),
            pltpu.VMEM((CHUNKS, half, width), f32),
            pltpu.VMEM((X_FIRST, NY, half, width), bf16),
            pltpu.VMEM((CHUNKS, NZ, own, width), f32),
            pltpu.VMEM((CHUNKS, 4, own, width), f32),
            pltpu.VMEM((CHUNKS, 15, own, width), f32),
            pltpu.VMEM((own, width), f32),
            pltpu.VMEM((2, 2, 128), f32),
            pltpu.VMEM((NZ - 1, 2, 128), f32),
            pltpu.VMEM((NY * NG * 2 - 1, 2, 128), f32),
            dma((6,)),
            dma((CHUNKS,)),
            dma((1,)),
            dma((CHUNKS, 3)),
            dma((2,)),
            dma((CHUNKS,)),
            dma((X_FIRST,)),
            dma((1,)),
            dma((CHUNKS, 3)),
            dma((2,)),
            dma((2,)),
            pltpu.SemaphoreType.REGULAR((2,)),
        ],
        compiler_params=pltpu.CompilerParams(
            collective_id=0, has_side_effects=True, vmem_limit_bytes=66_900_000
        ),
        name="reduce_deltas",
    )(token_ids, trigger, out_grad[0], hidden_acts[0], aggregate_prev[0], stale[0])
    aggregate, update, triggered = pl.pallas_call(
        output_kernel,
        out_shape=(
            jax.ShapeDtypeStruct((own, cols), f32),
            jax.ShapeDtypeStruct((own, cols), f32),
            jax.ShapeDtypeStruct((1, 1), f32),
        ),
        in_specs=[hbm] * 4,
        out_specs=(hbm,) * 3,
        scratch_shapes=[
            pltpu.VMEM((own, cols), f32),
            pltpu.VMEM((own, cols), f32),
            pltpu.VMEM((1, 1), f32),
            pltpu.VMEM((1, 1), f32),
            pltpu.VMEM((own, cols), f32),
            dma((7,)),
        ],
        compiler_params=pltpu.CompilerParams(vmem_limit_bytes=67_000_000),
        name="clip",
    )(total, aggregate_prev[0], factor, count)
    return (aggregate[None], update[None], triggered[0, 0])


def solution(mesh):
    in_specs = (
        P("dp", None, "shard"),
        P("dp", None, None),
        P("dp", None),
        P("dp", "shard"),
        P("dp", "shard", None),
        P("shard", "dp", None),
    )
    out_specs = (P("shard", "dp", None), P("shard", "dp", None), P())
    return jax.shard_map(local, mesh=mesh, in_specs=in_specs, out_specs=out_specs, check_vma=False)
```
